32 devices in a mesh: gx: 4 (over y, x), gy: 8 (over z, core).
Axes of the slice: x: 2, y: 2, z: 4, core: 2. Of those that a mesh axis runs over, the one named last changes fastest.
Arguments:
- density: float32 [32, 32, 128], P('gx', 'gy'), may hold values from -5 to 5
- susceptibility: float32 [32, 32, 128], P('gx', 'gy'), may hold values from -5 to 5
- station_cell: int32 [2, 1024], P(None, 'gx'), may hold values from 0 to 1023
- station_line: int32 [2, 1024], P(None, 'gx'), may hold values from 0 to 255, as said below
- observed: float32 [2, 1024], P(None, 'gx'), may hold values from -3 to 3
- data_weight: float32 [2, 1024], P(None, 'gx'), may hold values from 0.5 to 2
- trial_steps: float32 [8], replicated, may hold values from 0.05 to 0.5
Outputs:
- data_gradient: float32 [2, 32, 32, 128], P(None, 'gx', 'gy')
- cross_force: float32 [2, 32, 32, 128], P(None, 'gx', 'gy')
- weighted_residual: float32 [2, 1024], P(None, 'gx')
- trial_values: float32 [8], replicated
The draws below stay inside these ranges and needn't reach their ends.
Inputs may be any that keep to these rules, and one draw needn't show every extreme that they name: `station_line`: one or more survey lines hold no station of either field.
All inputs are finite; a program needn't handle non-finite values. Where the reference program divides by a largest or mean magnitude, that divisor is 1e-20 or more.
Results may differ from the reference program's by a relative error of at most 0.0003.
Values sent between devices are 32-bit elements; how exact they have to be, the bound alone decides.
A program may use at most 64 MiB of HBM per device.

```python
import math
import jax
import jax.numpy as jnp
from jax import lax

NZ = 128
LINES = 256
TRIALS = 8
NX = 32
NY = 32
STATIONS = 1024


def draw_density(key, part):
    return jnp.clip(jax.random.normal(key, (NX, NY, NZ), jnp.float32), -5.0, 5.0)


def draw_susceptibility(key, part):
    inner = jax.random.fold_in(key, 7)
    return jnp.clip(jax.random.normal(inner, (NX, NY, NZ), jnp.float32), -5.0, 5.0)


def draw_station_line(key, part):
    table_key = jax.random.fold_in(key, 11)
    pick_key = jax.random.fold_in(key, 12)
    missing_key = jax.random.fold_in(key, 13)
    table = jax.random.randint(table_key, (LINES,), 0, LINES, jnp.int32)
    missing = jax.random.randint(missing_key, (), 0, LINES, jnp.int32)
    table = jnp.where(table == missing, (table + 1) % LINES, table)
    picks = jax.random.randint(pick_key, (2, STATIONS), 0, LINES, jnp.int32)
    return table[picks]


def with_ends(result, key, least, high):
    longest = result.shape.index(max(result.shape))
    spots = []
    for shift in (0, 1):
        where = [jax.random.randint(jax.random.fold_in(key, axis), (), 0, length) for axis, length in enumerate(result.shape)]
        where[longest] = (where[longest] + shift) % result.shape[longest]
        spots.append(tuple(where))
    return result.at[spots[0]].set(least).at[spots[1]].set(high)


def steps_of(key, dims, shards, least, largest):
    loudness = 1.0
    for dim, shards_of in shards:
        heights = jax.random.uniform(jax.random.fold_in(jax.random.fold_in(key, 6), dim), (shards_of,), jnp.float32, least / len(shards), largest / len(shards))
        loudness = loudness * jnp.repeat(jnp.exp(heights), dims[dim] // shards_of).reshape((-1,) + (1,) * (len(dims) - 1 - dim))
    return loudness


def gaussian(stream_key, shape, width, limit, split=(), kind=jnp.bfloat16):
    entries = jax.random.normal(stream_key, shape, jnp.float32) * width
    if len(split) > 0:
        entries = steps_of(stream_key, shape, split, -0.22, 0.18) * entries
    return jnp.clip(entries, min=-limit, max=limit).astype(kind)


def setup_inputs(seed: int = 0) -> dict:
    streams_of = jax.random.split(jax.random.key(seed), 8)
    return {
        "density": draw_density(jax.random.fold_in(streams_of[7], 71), 0),
        "susceptibility": draw_susceptibility(jax.random.fold_in(streams_of[7], 71), 0),
        "station_cell": with_ends(jax.random.randint(streams_of[2], (2, STATIONS), 0, NX * NY), jax.random.fold_in(streams_of[2], 1), 0, (NX * NY) - 1).astype(jnp.int32),
        "station_line": draw_station_line(jax.random.fold_in(streams_of[7], 71), 0),
        "observed": gaussian(streams_of[4], (2, STATIONS), 0.5, 3.0, ((1, 4),), jnp.float32),
        "data_weight": jnp.clip(jnp.exp(math.log(2.0) - 1.3862944 * jax.random.uniform(streams_of[5], (2, STATIONS), jnp.float32) ** steps_of(streams_of[5], (2, STATIONS), ((1, 4),), -0.2, 0.2)), 0.5, 2.0),
        "trial_steps": jnp.clip(jnp.exp(jax.random.uniform(streams_of[6], (TRIALS,), jnp.float32, math.log(0.05), math.log(0.5))), 0.05, 0.5),
    }


cell_depth = 2.0
lift = 1.0
coupling_scale = 0.05
highest = lax.Precision.HIGHEST

def kernel_tile(field, station_x, station_y, cell_x, cell_y, depth):
    gap_x = station_x[:, None] - cell_x[None, :]
    gap_y = station_y[:, None] - cell_y[None, :]
    depth_row = depth[None, :]
    radius_sq = gap_x * gap_x + gap_y * gap_y + depth_row * depth_row
    inverse = lax.rsqrt(radius_sq)
    cube = inverse * inverse * inverse
    if field == 0:
        return depth_row * cube
    return (3.0 * depth_row * depth_row - radius_sq) * cube * inverse * inverse

def cell_coords(start, count):
    position = start + jnp.arange(count, dtype=jnp.int32)
    cell_x = (position // (NY * NZ)).astype(jnp.float32)
    cell_y = (position // NZ % NY).astype(jnp.float32)
    depth = ((position % NZ).astype(jnp.float32) + 0.5) * cell_depth + lift
    return (cell_x, cell_y, depth)

def forward_all(models, station_x, station_y):
    flat = models.reshape(2, -1)
    cells = flat.shape[1]
    block = math.gcd(cells, 8192)

    def turn(index, total):
        start = (index * block).astype(jnp.int32)
        cell_x, cell_y, depth = cell_coords(start, block)
        piece = lax.dynamic_slice_in_dim(flat, start, block, 1)
        rows = [jnp.dot(kernel_tile(field, station_x[field], station_y[field], cell_x, cell_y, depth), piece[field], precision=highest) for field in range(2)]
        return total + jnp.stack(rows)
    return lax.fori_loop(0, cells // block, turn, jnp.zeros((2, station_x.shape[1]), jnp.float32))

def adjoint_all(source, station_x, station_y):
    cells = NX * NY * NZ
    block = math.gcd(cells, 8192)

    def turn(index):
        start = (index * block).astype(jnp.int32)
        cell_x, cell_y, depth = cell_coords(start, block)
        rows = [jnp.dot(source[field], kernel_tile(field, station_x[field], station_y[field], cell_x, cell_y, depth), precision=highest) for field in range(2)]
        return jnp.stack(rows)
    parts = lax.map(turn, jnp.arange(cells // block, dtype=jnp.int32))
    return jnp.swapaxes(parts, 0, 1).reshape(2, NX, NY, NZ)

def forward_diffs(field):
    along_x = jnp.concatenate([field[1:] - field[:-1], jnp.zeros_like(field[:1])], axis=0)
    along_y = jnp.concatenate([field[:, 1:] - field[:, :-1], jnp.zeros_like(field[:, :1])], axis=1)
    along_z = jnp.concatenate([field[:, :, 1:] - field[:, :, :-1], jnp.zeros_like(field[:, :, :1])], axis=2)
    return (along_x, along_y, along_z)

def cross_energy(models):
    first_x, first_y, first_z = forward_diffs(models[0])
    second_x, second_y, second_z = forward_diffs(models[1])
    part_one = first_y * second_z - first_z * second_y
    part_two = first_z * second_x - first_x * second_z
    part_three = first_x * second_y - first_y * second_x
    return 0.5 * jnp.sum(part_one * part_one + part_two * part_two + part_three * part_three)

def level(values, lines):

    def one(value_row, line_row):
        sums = jax.ops.segment_sum(value_row, line_row, LINES)
        counts = jax.ops.segment_sum(jnp.ones_like(value_row), line_row, LINES)
        means = sums / jnp.maximum(counts, 1.0)
        return value_row - means[line_row]
    return jax.vmap(one)(values, lines)

def reference(density, susceptibility, station_cell, station_line, observed, data_weight, trial_steps):
    models = jnp.stack([density, susceptibility])
    station_x = (station_cell // NY).astype(jnp.float32)
    station_y = (station_cell % NY).astype(jnp.float32)
    total_stations = station_cell.shape[1]
    predicted = forward_all(models, station_x, station_y)
    residual = level(predicted - observed, station_line)
    weighted_residual = data_weight * residual
    source = level(data_weight * weighted_residual, station_line)
    data_gradient = adjoint_all(source, station_x, station_y)
    cross_force = jax.grad(cross_energy)(models)
    coupling = coupling_scale * total_stations / (NX * NY * NZ)
    gradient = data_gradient + coupling * cross_force
    peak = jnp.max(jnp.abs(gradient)) + 1e-06
    direction = gradient / peak
    image = forward_all(direction, station_x, station_y)
    change = level(image, station_line)
    values = []
    for trial in range(TRIALS):
        step = trial_steps[trial]
        moved = data_weight * (residual - step * change)
        values.append((0.5 * jnp.sum(moved * moved) + coupling * cross_energy(models - step * direction)) / (2 * total_stations))
    return (data_gradient, cross_force, weighted_residual, jnp.stack(values))
```

```python
import functools

import jax
import jax.numpy as jnp
from jax import lax
from jax.experimental import pallas as pl
from jax.experimental.pallas import tpu as pltpu
from jax.sharding import PartitionSpec as P

LINES = 256
LOW = 32
HIGH = LINES // LOW

cell_depth = 2.0
lift = 1.0
coupling_scale = 0.05

MESH = pl.DeviceIdType.MESH
f32 = jnp.float32
bf16 = jnp.bfloat16
NN = (((1,), (0,)), ((), ()))
NT = (((1,), (1,)), ((), ()))


def iota(shape, dim):
    return lax.broadcasted_iota(jnp.int32, shape, dim)


def split2(x):
    high = x.astype(bf16)
    return high, (x - high.astype(f32)).astype(bf16)


def split3(x):
    high = x.astype(bf16)
    rest = x - high.astype(f32)
    middle = rest.astype(bf16)
    return high, middle, (rest - middle.astype(f32)).astype(bf16)


def thirds(x):
    n = x.shape[0] // 3
    return x[:n] + x[n : 2 * n] + x[2 * n :]


def cross(a, b):
    return (a[1] * b[2] - a[2] * b[1], a[2] * b[0] - a[0] * b[2], a[0] * b[1] - a[1] * b[0])


def dot3(a, b):
    return a[0] * b[0] + a[1] * b[1] + a[2] * b[2]


def total(x):
    return jnp.sum(jnp.sum(x, axis=0, keepdims=True), axis=1, keepdims=True)


def largest(x):
    return jnp.max(jnp.max(x, axis=0, keepdims=True), axis=1, keepdims=True)


def kernel(
    G, C, den, sus, cell, line, obs, wgt, steps,
    dg_out, cf_out, wr_out, tv_out,
    E2, RS, F, A, cellb, lineb, obsb, wgtb, OY, OX, OHI, OLO, wrs,
    b1, b2, c1, c2, s1, s2, M, SH, RH, CH, CR, CFX, GE,
    s_st, r_st, s_h, r_h, s_c, r_c, s_b1, r_b1, s_b2, r_b2, s_c1, r_c1, s_c2, r_c2, s_s1, r_s1, s_s2, r_s2,
):
    R, W, K = den.shape
    own = cell.shape[1]
    NX, NY = R * G, W * C
    V = 2 * NY
    xp = 128 // V
    Q = NX // xp
    N = E2.shape[2]
    nch = N // 128
    ST = 2 * own * G
    T = steps.shape[0]
    mx = lax.axis_index("gx")
    my = lax.axis_index("gy")
    x0 = mx * R
    y0 = my * W
    total_stations = own * G
    coupling = coupling_scale * total_stations / (NX * NY * K)

    def at(dx, dy):
        return (lax.rem(mx + dx + G, G), lax.rem(my + dy + C, C))

    ycast = [at(0, d) for d in range(1, C)]
    xcast = [at(d, 0) for d in range(1, G)]
    diagonal = [at(1, -1), at(-1, 1)]
    barrier = pltpu.get_barrier_semaphore()
    partners = ycast + xcast + diagonal
    for where in partners:
        pl.semaphore_signal(barrier, inc=1, device_id=where, device_id_type=MESH)

    lane = iota((1, 128), 1)

    h_col = (iota((K, 128), 0).astype(f32) + 0.5) * cell_depth + lift
    h2 = h_col * h_col

    def table_turn(n, carry):
        gap_x = (n * xp + lane // V - 8 - x0).astype(f32)
        gap_y = (lane % V - 4 - y0).astype(f32)
        r2 = (gap_x * gap_x + gap_y * gap_y) + h2
        inverse = lax.rsqrt(r2)
        inverse2 = inverse * inverse
        cube = inverse2 * inverse
        both = (h_col * cube, (3.0 * h2 - r2) * cube * inverse2)
        spot = pl.ds(pl.multiple_of(n * 128, 128), 128)
        for f in range(2):
            high, low = split2(both[f])
            E2[f, 0:K, spot] = high
            E2[f, K : 2 * K, spot] = low
        return carry

    lax.fori_loop(0, nch, table_turn, 0)

    in_y = (lane % V) < NY

    def forward(columns, f):
        x = jnp.concatenate(columns, axis=0)
        high, low = split2(x)
        left = jnp.concatenate(
            [jnp.concatenate([high, high], axis=1), jnp.concatenate([low, low], axis=1)], axis=0
        )
        t = lax.dot_general(left, E2[f], NN, preferred_element_type=f32)
        t = t[: R * W] + t[R * W :]
        t2 = sum(pltpu.roll(t[j * R : (j + 1) * R], N - (4 - j), 1) for j in range(W))
        shifted = [t2] + [pltpu.roll(t2, N - c * V, 1) for c in range(1, xp)]
        sub = iota((R, NX * V), 0)
        acc = jnp.zeros((R, NX * V), f32)
        for i in range(R):
            s = 8 - i
            first = (s // xp) * 128
            acc = jnp.where(sub == i, shifted[s % xp][:, first : first + NX * V], acc)
        row = jnp.sum(acc, axis=0, keepdims=True)
        grid = jnp.concatenate([row[:, q * 128 : (q + 1) * 128] for q in range(Q)], axis=0)
        grid = jnp.where(in_y, grid, 0.0)
        return grid if f == 0 else pltpu.roll(grid, NY, 1)

    models = (den, sus)
    own_columns = [[models[f][:, j, :] for j in range(W)] for f in range(2)]
    b1[my] = forward(own_columns[0], 0) + forward(own_columns[1], 1)

    M[...] = jnp.zeros(M.shape, f32)
    F[...] = jnp.zeros(F.shape, f32)
    A[...] = jnp.zeros(A.shape, f32)
    CFX[...] = jnp.zeros(CFX.shape, f32)
    SH[...] = jnp.zeros(SH.shape, f32)
    CH[...] = jnp.zeros(CH.shape, f32)
    for f in range(2):
        for j in range(W):
            M[f, j + 1, 1 : R + 1, :] = own_columns[f][j]
        SH[0, f, 0:W, :] = models[f][R - 1]
        SH[1, f, 0:W, :] = models[f][0]
        SH[2, f, 0:R, :] = own_columns[f][W - 1]
        SH[3, f, 0:R, :] = own_columns[f][0]
        SH[4, f, 0:1, :] = models[f][R - 1, 0:1, :]
        SH[5, f, 0:1, :] = models[f][0, W - 1 : W, :]
    cellb[mx] = cell[...]
    lineb[mx] = line[...]
    obsb[mx] = obs[...]
    wgtb[mx] = wgt[...]

    pl.semaphore_wait(barrier, len(partners))

    def copy(src, dst, ssem, rsem, where):
        return pltpu.make_async_remote_copy(
            src_ref=src, dst_ref=dst, send_sem=ssem, recv_sem=rsem,
            device_id=where, device_id_type=MESH,
        )

    pending = []

    def share(buf, ssem, rsem, along_y):
        size, mine = (C, my) if along_y else (G, mx)
        for d, where in enumerate(ycast if along_y else xcast):
            one = copy(buf.at[mine], buf.at[mine], ssem.at[d], rsem.at[mine], where)
            one.start()
            pending.append(one)

    def arrived(buf, ssem, rsem, along_y):
        size, mine = (C, my) if along_y else (G, mx)
        for d in range(1, size):
            src = lax.rem(mine + d, size)
            copy(
                buf.at[src], buf.at[src], ssem.at[0], rsem.at[src],
                (ycast if along_y else xcast)[0],
            ).wait_recv()

    share(b1, s_b1, r_b1, True)
    station_bufs = (cellb, lineb, obsb, wgtb)
    for n, buf in enumerate(station_bufs):
        share(buf, s_st.at[n], r_st.at[n], False)
    halo_targets = [at(1, 0), at(-1, 0), at(0, 1), at(0, -1), at(1, -1), at(-1, 1)]
    halos = []
    for n, where in enumerate(halo_targets):
        one = copy(SH.at[n], RH.at[n], s_h.at[n], r_h.at[n], where)
        one.start()
        halos.append(one)
        pending.append(one)

    for n, buf in enumerate(station_bufs):
        arrived(buf, s_st.at[n], r_st.at[n], False)

    def spread_out(buf):
        return jnp.concatenate([buf[g, f : f + 1, :] for g in range(G) for f in range(2)], axis=1)

    field_of = (iota((1, ST), 1) // own) % 2
    cells = spread_out(cellb)
    lines = spread_out(lineb)
    observed = spread_out(obsb)
    weight = spread_out(wgtb)
    at_x = cells // NY
    at_y = cells - at_x * NY
    key_lane = (at_x % xp) * V + field_of * NY + at_y
    key_row = at_x // xp
    OY[...] = jnp.where(iota((128, ST), 0) == key_lane, 1.0, 0.0).astype(bf16)
    OX[...] = jnp.where(iota((Q, ST), 0) == key_row, 1.0, 0.0)
    OHI[...] = jnp.where(iota((2 * HIGH, ST), 0) == field_of * HIGH + lines // LOW, 1.0, 0.0)
    OLO[...] = jnp.where(iota((LOW, ST), 0) == lines % LOW, 1.0, 0.0).astype(bf16)
    counts = lax.dot_general(OHI[...].astype(bf16), OLO[...], NT, preferred_element_type=f32)
    per_line = 1.0 / jnp.maximum(counts, 1.0)

    def by_row(mask, v):
        return jnp.concatenate([(mask * p.astype(f32)).astype(bf16) for p in split3(v)], axis=0)

    def project(v):
        sums = lax.dot_general(by_row(OHI[...], v), OLO[...], NT, preferred_element_type=f32)
        means = thirds(sums) * per_line
        parts = jnp.concatenate(split3(means), axis=0)
        back = lax.dot_general(parts, OLO[...], NN, preferred_element_type=f32)
        return jnp.sum(thirds(back) * OHI[...], axis=0, keepdims=True)

    def at_stations(grid):
        parts = jnp.concatenate(split3(grid), axis=0)
        back = lax.dot_general(parts, OY[...], NN, preferred_element_type=f32)
        return jnp.sum(thirds(back) * OX[...], axis=0, keepdims=True)

    arrived(b1, s_b1, r_b1, True)
    partial = b1[0]
    for n in range(1, C):
        partial = partial + b1[n]
    b2[mx] = partial
    share(b2, s_b2, r_b2, False)

    for one in halos:
        one.wait_recv()
    for f in range(2):
        for j in range(W):
            M[f, j + 1, 0:1, :] = RH[0, f, j : j + 1, :]
            M[f, j + 1, R + 1 : R + 2, :] = RH[1, f, j : j + 1, :]
        M[f, 0, 1 : R + 1, :] = RH[2, f, 0:R, :]
        M[f, W + 1, 1 : R + 1, :] = RH[3, f, 0:R, :]
        M[f, W + 1, 0:1, :] = RH[4, f, 0:1, :]
        M[f, 0, R + 1 : R + 2, :] = RH[5, f, 0:1, :]
    mask_z = (iota((1, K), 1) < K - 1).astype(f32)

    def diffs(ref, f, c, row, count, global_x, global_y):
        base = ref[f, c, row : row + count, :]
        up = ref[f, c, row + 1 : row + 1 + count, :]
        right = ref[f, c + 1, row : row + count, :]
        keep_x = (global_x < NX - 1).astype(f32)
        keep_y = (global_y < NY - 1).astype(f32)
        return (
            (up - base) * keep_x,
            (right - base) * keep_y,
            (pltpu.roll(base, K - 1, 1) - base) * mask_z,
        )

    gx_rim = x0 - 1 + iota((16, K), 0)
    before = [None, None]
    for c in range(W + 1):
        gy_rim = y0 - 1 + c + jnp.zeros((16, K), jnp.int32)
        a = diffs(M, 0, c, 0, 16, gx_rim, gy_rim)
        b = diffs(M, 1, c, 0, 16, gx_rim, gy_rim)
        valid = ((gx_rim >= 0) & (gy_rim >= 0)).astype(f32)
        t = tuple(part * valid for part in cross(a, b))
        keep_x = (gx_rim < NX - 1).astype(f32)
        keep_y = (gy_rim < NY - 1).astype(f32)
        for f, force in enumerate((cross(b, t), cross(t, a))):
            fx, fy, fz = force[0] * keep_x, force[1] * keep_y, force[2] * mask_z
            if c > 0:
                d = before[f] - fy - fx + pltpu.roll(fz, 1, 1) - fz
                result = pltpu.roll(d, 15, 0)[0:R] + fx[0:R]
                CFX[f, c - 1, 0:R, :] = result
                cf_out[f, :, c - 1, :] = result
                CH[0, f, c - 1 : c, :] = result[0:1]
                if c == 1:
                    CH[1, f, 0:R, :] = result
            before[f] = fy
    force_halos = []
    for n, where in enumerate((at(-1, 0), at(0, -1))):
        one = copy(CH.at[n], CR.at[n], s_c.at[n], r_c.at[n], where)
        one.start()
        force_halos.append(one)
        pending.append(one)

    arrived(b2, s_b2, r_b2, False)
    grid = b2[0]
    for n in range(1, G):
        grid = grid + b2[n]

    misfit = at_stations(grid) - observed
    residual = misfit - project(misfit)
    weighted = weight * residual
    wrs[...] = weighted
    source = weight * weighted
    source = source - project(source)
    S = thirds(
        lax.dot_general(by_row(OX[...], source), OY[...], NT, preferred_element_type=f32)
    )

    for one in force_halos:
        one.wait_recv()
    for f in range(2):
        for j in range(W):
            CFX[f, j, R : R + 1, :] = CR[0, f, j : j + 1, :]
        CFX[f, W, 0:R, :] = CR[1, f, 0:R, :]

    for f in range(2):
        S_f = jnp.where(in_y, S if f == 0 else pltpu.roll(S, 128 - NY, 1), 0.0)
        A[f, 8 : 8 + Q, :] = S_f
        for j in range(W + 1):
            now = A[f, 7 : 7 + Q + 8, :]
            later = A[f, 8 : 8 + Q + 8, :]
            for c in range(xp):
                turn = (4 - j + 128 - c * V) % 128
                first = now if turn == 0 else pltpu.roll(now, turn, 1)
                second = later if turn == 0 else pltpu.roll(later, turn, 1)
                value = first if c == 0 else jnp.where(lane < 128 - c * V, first, second)
                high, low = split2(value)
                rows = pl.ds(8 - xp + c, Q + 8, stride=xp) if xp > 1 else pl.ds(7, Q + 8)
                F[f, j, 0, rows, :] = high.astype(f32)
                F[f, j, 1, rows, :] = low.astype(f32)
        for j in range(W + 1):
            for h in range(2):
                for n in range(nch):
                    RS[f, (h * (W + 1) + j) * 16 : (h * (W + 1) + j + 1) * 16, n * 128 : (n + 1) * 128] = F[
                        f, j, h, n * xp : n * xp + 16, :
                    ].astype(bf16)
        D = lax.dot_general(RS[f], E2[f], NT, preferred_element_type=f32)
        half = (W + 1) * 16
        D = D[:half] + D[half:]
        D = D[:, :K] + D[:, K:]
        for j in range(W + 1):
            piece = D[j * 16 : (j + 1) * 16]
            GE[f, j, 0:16, :] = piece + coupling * CFX[f, j]
            if j < W:
                dg_out[f, :, j, :] = piece[0:R]

    g_columns = [[GE[f, j, 0:R, :] for j in range(W)] for f in range(2)]
    c1[my] = forward(g_columns[0], 0) + forward(g_columns[1], 1)
    share(c1, s_c1, r_c1, True)

    sub16 = iota((16, K), 0)
    own_peak = functools.reduce(
        jnp.maximum, [jnp.abs(g_columns[f][j]) for f in range(2) for j in range(W)]
    )
    rim_peak = functools.reduce(
        jnp.maximum,
        [jnp.where(sub16 <= R, jnp.abs(GE[f, j, 0:16, :]), 0.0) for f in range(2) for j in range(W + 1)],
    )
    own_peak = largest(own_peak) + 1e-06
    scale = largest(rim_peak) + 1e-06
    for f in range(2):
        for j in range(W + 1):
            GE[f, j, 0:16, :] = GE[f, j, 0:16, :] / scale
    gx_own = x0 + iota((R, K), 0)
    powers = [jnp.zeros((R, K), f32) for _ in range(5)]
    for j in range(W):
        gy_own = y0 + j + jnp.zeros((R, K), jnp.int32)
        a = diffs(M, 0, j + 1, 1, R, gx_own, gy_own)
        b = diffs(M, 1, j + 1, 1, R, gx_own, gy_own)
        da = diffs(GE, 0, j, 0, R, gx_own, gy_own)
        db = diffs(GE, 1, j, 0, R, gx_own, gy_own)
        u = cross(a, b)
        v = tuple(p + q for p, q in zip(cross(da, b), cross(a, db)))
        w = cross(da, db)
        powers[0] += dot3(u, u)
        powers[1] -= 2.0 * dot3(u, v)
        powers[2] += dot3(v, v) + 2.0 * dot3(u, w)
        powers[3] -= 2.0 * dot3(v, w)
        powers[4] += dot3(w, w)
    scalars = [own_peak, scale] + [total(p) for p in powers]
    lane8 = iota((8, 128), 1)
    message = jnp.zeros((8, 128), f32)
    for n, value in enumerate(scalars):
        message = jnp.where(lane8 == n, value, message)
    s1[my] = message
    share(s1, s_s1, r_s1, True)

    arrived(c1, s_c1, r_c1, True)
    partial = c1[0]
    for n in range(1, C):
        partial = partial + c1[n]
    c2[mx] = partial
    share(c2, s_c2, r_c2, False)
    arrived(s1, s_s1, r_s1, True)
    s2[mx] = jnp.concatenate([s1[n, 0:1, :] for n in range(C)], axis=0)
    share(s2, s_s2, r_s2, False)

    chunk = 2 * own
    mine = wrs[0:1, pl.ds(pl.multiple_of(mx * chunk, 128), chunk)]
    for f in range(2):
        wr_out[f : f + 1, :] = mine[:, f * own : (f + 1) * own]

    arrived(c2, s_c2, r_c2, False)
    grid = c2[0]
    for n in range(1, G):
        grid = grid + c2[n]
    image = at_stations(grid)
    change = image - project(image)

    arrived(s2, s_s2, r_s2, False)
    table = jnp.concatenate([s2[n] for n in range(G)], axis=0)
    peak = jnp.max(table[:, 0:1], axis=0, keepdims=True)
    change = change / peak
    sub_t = iota((T, 128), 0)
    step_rows = jnp.zeros((T, 128), f32)
    step_lanes = jnp.zeros((1, 128), f32)
    for k in range(T):
        step_rows = jnp.where(sub_t == k, steps[k], step_rows)
        step_lanes = jnp.where(lane == k, steps[k], step_lanes)
    moved = weight * (residual - step_rows[:, 0:1] * change)
    data = 0.5 * jnp.sum(moved * moved, axis=1, keepdims=True)
    data = jnp.sum(jnp.where(iota((T, 128), 1) == sub_t, data, 0.0), axis=0, keepdims=True)
    tau = step_lanes * (table[:, 1:2] / peak)
    energy = table[:, 6:7] * tau
    for n in (5, 4, 3):
        energy = (energy + table[:, n : n + 1]) * tau
    energy = energy + table[:, 2:3]
    energy = 0.5 * jnp.sum(energy, axis=0, keepdims=True)
    values = (data + coupling * energy) / (2 * total_stations)
    tv_out[...] = values[:, 0:T]

    for one in pending:
        one.wait_send()


def body(G, C, density, susceptibility, station_cell, station_line, observed, data_weight, trial_steps):
    R, W, K = density.shape
    own = station_cell.shape[1]
    NX, NY = R * G, W * C
    V = 2 * NY
    xp = 128 // V
    Q = NX // xp
    N = (NX + 8) * V
    ST = 2 * own * G
    T = trial_steps.shape[0]
    vmem = pl.BlockSpec(memory_space=pltpu.VMEM)
    dma = pltpu.SemaphoreType.DMA
    scratch = [
        pltpu.VMEM((2, 2 * K, N), bf16),
        pltpu.VMEM((2, 2 * (W + 1) * 16, N), bf16),
        pltpu.VMEM((2, W + 1, 2, NX + 24, 128), f32),
        pltpu.VMEM((2, Q + 16, 128), f32),
        pltpu.VMEM((G, 2, own), jnp.int32),
        pltpu.VMEM((G, 2, own), jnp.int32),
        pltpu.VMEM((G, 2, own), f32),
        pltpu.VMEM((G, 2, own), f32),
        pltpu.VMEM((128, ST), bf16),
        pltpu.VMEM((Q, ST), f32),
        pltpu.VMEM((2 * HIGH, ST), f32),
        pltpu.VMEM((LOW, ST), bf16),
        pltpu.VMEM((1, ST), f32),
        pltpu.VMEM((C, Q, 128), f32),
        pltpu.VMEM((G, Q, 128), f32),
        pltpu.VMEM((C, Q, 128), f32),
        pltpu.VMEM((G, Q, 128), f32),
        pltpu.VMEM((C, 8, 128), f32),
        pltpu.VMEM((G, C, 128), f32),
        pltpu.VMEM((2, W + 2, 24, K), f32),
        pltpu.VMEM((6, 2, 8, K), f32),
        pltpu.VMEM((6, 2, 8, K), f32),
        pltpu.VMEM((2, 2, 8, K), f32),
        pltpu.VMEM((2, 2, 8, K), f32),
        pltpu.VMEM((2, W + 1, 16, K), f32),
        pltpu.VMEM((2, W + 1, 24, K), f32),
        dma((4, G)), dma((4, G)),
        dma((6,)), dma((6,)),
        dma((2,)), dma((2,)),
        dma((C,)), dma((C,)),
        dma((G,)), dma((G,)),
        dma((C,)), dma((C,)),
        dma((G,)), dma((G,)),
        dma((C,)), dma((C,)),
        dma((G,)), dma((G,)),
    ]
    out = pl.pallas_call(
        functools.partial(kernel, G, C),
        out_shape=(
            jax.ShapeDtypeStruct((2, R, W, K), f32),
            jax.ShapeDtypeStruct((2, R, W, K), f32),
            jax.ShapeDtypeStruct((2, own), f32),
            jax.ShapeDtypeStruct((1, T), f32),
        ),
        in_specs=[vmem] * 6 + [pl.BlockSpec(memory_space=pltpu.SMEM)],
        out_specs=(vmem,) * 4,
        scratch_shapes=scratch,
        compiler_params=pltpu.CompilerParams(
            collective_id=0, has_side_effects=True, vmem_limit_bytes=56 * 1024 * 1024
        ),
    )(density, susceptibility, station_cell, station_line, observed, data_weight, trial_steps)
    return out[0], out[1], out[2], out[3].reshape(-1)


def solution(mesh):
    placed = (
        P("gx", "gy", None),
        P("gx", "gy", None),
        P(None, "gx"),
        P(None, "gx"),
        P(None, "gx"),
        P(None, "gx"),
        P(),
    )
    return jax.shard_map(
        functools.partial(body, mesh.shape["gx"], mesh.shape["gy"]),
        mesh=mesh,
        in_specs=placed,
        out_specs=(P(None, "gx", "gy", None), P(None, "gx", "gy", None), P(None, "gx"), P()),
        check_vma=False,
    )
```

```python
import functools

import jax
import jax.numpy as jnp
from jax import lax
from jax.experimental import pallas as pl
from jax.experimental.pallas import tpu as pltpu
from jax.sharding import PartitionSpec as P

LINES = 256
LOW = 32
CORES = 2
HIGH = LINES // LOW

cell_depth = 2.0
lift = 1.0
coupling_scale = 0.05

MESH = pl.DeviceIdType.MESH
f32 = jnp.float32
bf16 = jnp.bfloat16
NN = (((1,), (0,)), ((), ()))
NT = (((1,), (1,)), ((), ()))


def iota(shape, dim):
    return lax.broadcasted_iota(jnp.int32, shape, dim)


def split2(x):
    high = x.astype(bf16)
    return high, (x - high.astype(f32)).astype(bf16)


def split3(x):
    high = x.astype(bf16)
    rest = x - high.astype(f32)
    middle = rest.astype(bf16)
    return high, middle, (rest - middle.astype(f32)).astype(bf16)


def thirds(x):
    n = x.shape[0] // 3
    return x[:n] + x[n : 2 * n] + x[2 * n :]


def cross(a, b):
    return (a[1] * b[2] - a[2] * b[1], a[2] * b[0] - a[0] * b[2], a[0] * b[1] - a[1] * b[0])


def dot3(a, b):
    return a[0] * b[0] + a[1] * b[1] + a[2] * b[2]


def total(x):
    return jnp.sum(jnp.sum(x, axis=0, keepdims=True), axis=1, keepdims=True)


def largest(x):
    return jnp.max(jnp.max(x, axis=0, keepdims=True), axis=1, keepdims=True)


def kernel(
    G, C, den_in, sus_in, cell_in, line_in, obs_in, wgt_in, steps_in,
    dg_out, cf_out, wr_out, tv_out,
    den, sus, steps, s_in, E2, RS, F, A, cellb, lineb, obsb, wgtb, OY, OX, OHI, OLO, wrs,
    b1, b2, c1, c2, s1, s2, M, SH, RH, CH, CR, CFX, GE,
    s_st, r_st, s_h, r_h, s_c, r_c, s_b1, r_b1, s_b2, r_b2, s_c1, r_c1, s_c2, r_c2, s_s1, r_s1, s_s2, r_s2,
):
    R, W, K = den.shape
    own = cell_in.shape[1]
    NX, NY = R * G, W * C
    V = 2 * NY
    xp = 128 // V
    Q = NX // xp
    N = E2.shape[2]
    nch = N // 128
    ST = 2 * own * G
    T = steps.shape[0]
    mx = lax.axis_index("gx")
    my = lax.axis_index("gy")
    x0 = mx * R
    y0 = my * W
    total_stations = own * G
    coupling = coupling_scale * total_stations / (NX * NY * K)

    def at(dx, dy):
        return (lax.rem(mx + dx + G, G), lax.rem(my + dy + C, C))

    Z = C // CORES
    chip, core = my // CORES, lax.rem(my, CORES)
    zcast = [at(0, CORES * d) for d in range(1, Z)]
    xcast = [at(d, 0) for d in range(1, G)]
    gcast = xcast + [
        (lax.rem(mx + d, G), chip * CORES + lax.rem(core + e, CORES)) for e in range(1, CORES) for d in range(G)
    ]
    groups = {
        "z": (zcast, chip, [lax.rem(chip + d, Z) for d in range(1, Z)]),
        "x": (xcast, mx, [lax.rem(mx + d, G) for d in range(1, G)]),
        "g": (
            gcast,
            mx * CORES + core,
            [lax.rem(mx + d, G) * CORES + core for d in range(1, G)]
            + [
                lax.rem(mx + d, G) * CORES + lax.rem(core + e, CORES)
                for e in range(1, CORES)
                for d in range(G)
            ],
        ),
    }
    slot = mx * CORES + core
    barrier = pltpu.get_barrier_semaphore()
    partners = zcast + gcast + [at(0, 1), at(0, -1), at(1, -1), at(-1, 1)]
    for where in partners:
        pl.semaphore_signal(barrier, inc=1, device_id=where, device_id_type=MESH)

    loads = [
        pltpu.make_async_copy(src, dst, s_in.at[n])
        for n, (src, dst) in enumerate(
            (
                (den_in, den),
                (sus_in, sus),
                (cell_in, cellb.at[mx]),
                (line_in, lineb.at[mx]),
                (obs_in, obsb.at[mx]),
                (wgt_in, wgtb.at[mx]),
                (steps_in, steps),
            )
        )
    ]
    for one in loads:
        one.start()

    lane = iota((1, 128), 1)

    h_col = (iota((K, 128), 0).astype(f32) + 0.5) * cell_depth + lift
    h2 = h_col * h_col

    def table_turn(n, carry):
        gap_x = (n * xp + lane // V - 8 - x0).astype(f32)
        gap_y = (lane % V - 4 - y0).astype(f32)
        r2 = (gap_x * gap_x + gap_y * gap_y) + h2
        inverse = lax.rsqrt(r2)
        inverse2 = inverse * inverse
        cube = inverse2 * inverse
        both = (h_col * cube, (3.0 * h2 - r2) * cube * inverse2)
        spot = pl.ds(pl.multiple_of(n * 128, 128), 128)
        for f in range(2):
            high, low = split2(both[f])
            E2[f, 0:K, spot] = high
            E2[f, K : 2 * K, spot] = low
        return carry

    lax.fori_loop(0, nch, table_turn, 0)

    in_y = (lane % V) < NY

    def forward(columns, f):
        x = jnp.concatenate(columns, axis=0)
        high, low = split2(x)
        left = jnp.concatenate(
            [jnp.concatenate([high, high], axis=1), jnp.concatenate([low, low], axis=1)], axis=0
        )
        t = lax.dot_general(left, E2[f], NN, preferred_element_type=f32)
        t = t[: R * W] + t[R * W :]
        t2 = sum(pltpu.roll(t[j * R : (j + 1) * R], N - (4 - j), 1) for j in range(W))
        shifted = [t2] + [pltpu.roll(t2, N - c * V, 1) for c in range(1, xp)]
        sub = iota((R, NX * V), 0)
        acc = jnp.zeros((R, NX * V), f32)
        for i in range(R):
            s = 8 - i
            first = (s // xp) * 128
            acc = jnp.where(sub == i, shifted[s % xp][:, first : first + NX * V], acc)
        row = jnp.sum(acc, axis=0, keepdims=True)
        grid = jnp.concatenate([row[:, q * 128 : (q + 1) * 128] for q in range(Q)], axis=0)
        grid = jnp.where(in_y, grid, 0.0)
        return grid if f == 0 else pltpu.roll(grid, NY, 1)

    for one in loads[:2]:
        one.wait()
    models = (den, sus)
    own_columns = [[models[f][:, j, :] for j in range(W)] for f in range(2)]
    b1[chip] = forward(own_columns[0], 0) + forward(own_columns[1], 1)

    M[...] = jnp.zeros(M.shape, f32)
    F[...] = jnp.zeros(F.shape, f32)
    A[...] = jnp.zeros(A.shape, f32)
    CFX[...] = jnp.zeros(CFX.shape, f32)
    SH[...] = jnp.zeros(SH.shape, f32)
    CH[...] = jnp.zeros(CH.shape, f32)
    s2[slot] = jnp.zeros(s2.shape[1:], f32)
    for f in range(2):
        for j in range(W):
            M[f, j + 1, 1 : R + 1, :] = own_columns[f][j]
        SH[0, f, 0:W, :] = models[f][R - 1]
        SH[1, f, 0:W, :] = models[f][0]
        SH[2, f, 0:R, :] = own_columns[f][W - 1]
        SH[3, f, 0:R, :] = own_columns[f][0]
        SH[4, f, 0:1, :] = models[f][R - 1, 0:1, :]
        SH[5, f, 0:1, :] = models[f][0, W - 1 : W, :]
    for one in loads[2:]:
        one.wait()

    pl.semaphore_wait(barrier, len(partners))

    def copy(src, dst, ssem, rsem, where):
        return pltpu.make_async_remote_copy(
            src_ref=src, dst_ref=dst, send_sem=ssem, recv_sem=rsem,
            device_id=where, device_id_type=MESH,
        )

    pending = []

    def share(buf, ssem, rsem, group):
        targets, mine, _ = groups[group]
        for d, where in enumerate(targets):
            one = copy(buf.at[mine], buf.at[mine], ssem.at[d], rsem.at[mine], where)
            one.start()
            pending.append(one)

    def arrived(buf, ssem, rsem, group):
        targets, _, sources = groups[group]
        for src in sources:
            copy(buf.at[src], buf.at[src], ssem.at[0], rsem.at[src], targets[0]).wait_recv()

    share(b1, s_b1, r_b1, "z")
    station_bufs = (cellb, lineb, obsb, wgtb)
    for n, buf in enumerate(station_bufs):
        share(buf, s_st.at[n], r_st.at[n], "x")
    halo_targets = [at(1, 0), at(-1, 0), at(0, 1), at(0, -1), at(1, -1), at(-1, 1)]
    halos = []
    for n, where in enumerate(halo_targets):
        one = copy(SH.at[n], RH.at[n], s_h.at[n], r_h.at[n], where)
        one.start()
        halos.append(one)
        pending.append(one)

    for n, buf in enumerate(station_bufs):
        arrived(buf, s_st.at[n], r_st.at[n], "x")

    def spread_out(buf):
        return jnp.concatenate([buf[g, f : f + 1, :] for g in range(G) for f in range(2)], axis=1)

    field_of = (iota((1, ST), 1) // own) % 2
    cells = spread_out(cellb)
    lines = spread_out(lineb)
    observed = spread_out(obsb)
    weight = spread_out(wgtb)
    at_x = cells // NY
    at_y = cells - at_x * NY
    key_lane = (at_x % xp) * V + field_of * NY + at_y
    key_row = at_x // xp
    OY[...] = jnp.where(iota((128, ST), 0) == key_lane, 1.0, 0.0).astype(bf16)
    OX[...] = jnp.where(iota((Q, ST), 0) == key_row, 1.0, 0.0)
    OHI[...] = jnp.where(iota((2 * HIGH, ST), 0) == field_of * HIGH + lines // LOW, 1.0, 0.0)
    OLO[...] = jnp.where(iota((LOW, ST), 0) == lines % LOW, 1.0, 0.0).astype(bf16)
    counts = lax.dot_general(OHI[...].astype(bf16), OLO[...], NT, preferred_element_type=f32)
    per_line = 1.0 / jnp.maximum(counts, 1.0)

    def by_row(mask, v):
        return jnp.concatenate([(mask * p.astype(f32)).astype(bf16) for p in split3(v)], axis=0)

    def project(v):
        sums = lax.dot_general(by_row(OHI[...], v), OLO[...], NT, preferred_element_type=f32)
        means = thirds(sums) * per_line
        parts = jnp.concatenate(split3(means), axis=0)
        back = lax.dot_general(parts, OLO[...], NN, preferred_element_type=f32)
        return jnp.sum(thirds(back) * OHI[...], axis=0, keepdims=True)

    def at_stations(grid):
        parts = jnp.concatenate(split3(grid), axis=0)
        back = lax.dot_general(parts, OY[...], NN, preferred_element_type=f32)
        return jnp.sum(thirds(back) * OX[...], axis=0, keepdims=True)

    arrived(b1, s_b1, r_b1, "z")
    partial = b1[0]
    for n in range(1, Z):
        partial = partial + b1[n]
    b2[slot] = partial
    share(b2, s_b2, r_b2, "g")

    for one in halos:
        one.wait_recv()
    for f in range(2):
        for j in range(W):
            M[f, j + 1, 0:1, :] = RH[0, f, j : j + 1, :]
            M[f, j + 1, R + 1 : R + 2, :] = RH[1, f, j : j + 1, :]
        M[f, 0, 1 : R + 1, :] = RH[2, f, 0:R, :]
        M[f, W + 1, 1 : R + 1, :] = RH[3, f, 0:R, :]
        M[f, W + 1, 0:1, :] = RH[4, f, 0:1, :]
        M[f, 0, R + 1 : R + 2, :] = RH[5, f, 0:1, :]
    mask_z = (iota((1, K), 1) < K - 1).astype(f32)

    def diffs(ref, f, c, row, count, global_x, global_y):
        base = ref[f, c, row : row + count, :]
        up = ref[f, c, row + 1 : row + 1 + count, :]
        right = ref[f, c + 1, row : row + count, :]
        keep_x = (global_x < NX - 1).astype(f32)
        keep_y = (global_y < NY - 1).astype(f32)
        return (
            (up - base) * keep_x,
            (right - base) * keep_y,
            (pltpu.roll(base, K - 1, 1) - base) * mask_z,
        )

    gx_rim = x0 - 1 + iota((16, K), 0)
    before = [None, None]
    for c in range(W + 1):
        gy_rim = y0 - 1 + c + jnp.zeros((16, K), jnp.int32)
        a = diffs(M, 0, c, 0, 16, gx_rim, gy_rim)
        b = diffs(M, 1, c, 0, 16, gx_rim, gy_rim)
        valid = ((gx_rim >= 0) & (gy_rim >= 0)).astype(f32)
        t = tuple(part * valid for part in cross(a, b))
        keep_x = (gx_rim < NX - 1).astype(f32)
        keep_y = (gy_rim < NY - 1).astype(f32)
        for f, force in enumerate((cross(b, t), cross(t, a))):
            fx, fy, fz = force[0] * keep_x, force[1] * keep_y, force[2] * mask_z
            if c > 0:
                d = before[f] - fy - fx + pltpu.roll(fz, 1, 1) - fz
                result = pltpu.roll(d, 15, 0)[0:R] + fx[0:R]
                CFX[f, c - 1, 0:R, :] = result
                cf_out[f, :, c - 1, :] = result
                CH[0, f, c - 1 : c, :] = result[0:1]
                if c == 1:
                    CH[1, f, 0:R, :] = result
            before[f] = fy
    force_halos = []
    for n, where in enumerate((at(-1, 0), at(0, -1))):
        one = copy(CH.at[n], CR.at[n], s_c.at[n], r_c.at[n], where)
        one.start()
        force_halos.append(one)
        pending.append(one)

    arrived(b2, s_b2, r_b2, "g")
    grid = b2[0]
    for n in range(1, CORES * G):
        grid = grid + b2[n]

    misfit = at_stations(grid) - observed
    residual = misfit - project(misfit)
    weighted = weight * residual
    wrs[...] = weighted
    source = weight * weighted
    source = source - project(source)
    S = thirds(
        lax.dot_general(by_row(OX[...], source), OY[...], NT, preferred_element_type=f32)
    )

    for one in force_halos:
        one.wait_recv()
    for f in range(2):
        for j in range(W):
            CFX[f, j, R : R + 1, :] = CR[0, f, j : j + 1, :]
        CFX[f, W, 0:R, :] = CR[1, f, 0:R, :]

    for f in range(2):
        S_f = jnp.where(in_y, S if f == 0 else pltpu.roll(S, 128 - NY, 1), 0.0)
        A[f, 8 : 8 + Q, :] = S_f
        for j in range(W + 1):
            now = A[f, 7 : 7 + Q + 8, :]
            later = A[f, 8 : 8 + Q + 8, :]
            for c in range(xp):
                turn = (4 - j + 128 - c * V) % 128
                first = now if turn == 0 else pltpu.roll(now, turn, 1)
                second = later if turn == 0 else pltpu.roll(later, turn, 1)
                value = first if c == 0 else jnp.where(lane < 128 - c * V, first, second)
                high, low = split2(value)
                rows = pl.ds(8 - xp + c, Q + 8, stride=xp) if xp > 1 else pl.ds(7, Q + 8)
                F[f, j, 0, rows, :] = high.astype(f32)
                F[f, j, 1, rows, :] = low.astype(f32)
        for j in range(W + 1):
            for h in range(2):
                for n in range(nch):
                    RS[f, (h * (W + 1) + j) * 16 : (h * (W + 1) + j + 1) * 16, n * 128 : (n + 1) * 128] = F[
                        f, j, h, n * xp : n * xp + 16, :
                    ].astype(bf16)
        D = lax.dot_general(RS[f], E2[f], NT, preferred_element_type=f32)
        half = (W + 1) * 16
        D = D[:half] + D[half:]
        D = D[:, :K] + D[:, K:]
        for j in range(W + 1):
            piece = D[j * 16 : (j + 1) * 16]
            GE[f, j, 0:16, :] = piece + coupling * CFX[f, j]
            if j < W:
                dg_out[f, :, j, :] = piece[0:R]

    g_columns = [[GE[f, j, 0:R, :] for j in range(W)] for f in range(2)]
    c1[chip] = forward(g_columns[0], 0) + forward(g_columns[1], 1)
    share(c1, s_c1, r_c1, "z")

    sub16 = iota((16, K), 0)
    own_peak = functools.reduce(
        jnp.maximum, [jnp.abs(g_columns[f][j]) for f in range(2) for j in range(W)]
    )
    rim_peak = functools.reduce(
        jnp.maximum,
        [jnp.where(sub16 <= R, jnp.abs(GE[f, j, 0:16, :]), 0.0) for f in range(2) for j in range(W + 1)],
    )
    own_peak = largest(own_peak) + 1e-06
    scale = largest(rim_peak) + 1e-06
    for f in range(2):
        for j in range(W + 1):
            GE[f, j, 0:16, :] = GE[f, j, 0:16, :] / scale
    gx_own = x0 + iota((R, K), 0)
    powers = [jnp.zeros((R, K), f32) for _ in range(5)]
    for j in range(W):
        gy_own = y0 + j + jnp.zeros((R, K), jnp.int32)
        a = diffs(M, 0, j + 1, 1, R, gx_own, gy_own)
        b = diffs(M, 1, j + 1, 1, R, gx_own, gy_own)
        da = diffs(GE, 0, j, 0, R, gx_own, gy_own)
        db = diffs(GE, 1, j, 0, R, gx_own, gy_own)
        u = cross(a, b)
        v = tuple(p + q for p, q in zip(cross(da, b), cross(a, db)))
        w = cross(da, db)
        powers[0] += dot3(u, u)
        powers[1] -= 2.0 * dot3(u, v)
        powers[2] += dot3(v, v) + 2.0 * dot3(u, w)
        powers[3] -= 2.0 * dot3(v, w)
        powers[4] += dot3(w, w)
    scalars = [own_peak, scale] + [total(p) for p in powers]
    lane8 = iota((8, 128), 1)
    message = jnp.zeros((8, 128), f32)
    for n, value in enumerate(scalars):
        message = jnp.where(lane8 == n, value, message)
    s1[chip] = message
    share(s1, s_s1, r_s1, "z")

    arrived(c1, s_c1, r_c1, "z")
    partial = c1[0]
    for n in range(1, Z):
        partial = partial + c1[n]
    c2[slot] = partial
    share(c2, s_c2, r_c2, "g")
    arrived(s1, s_s1, r_s1, "z")
    s2[slot, 0:Z, :] = jnp.concatenate([s1[n, 0:1, :] for n in range(Z)], axis=0)
    share(s2, s_s2, r_s2, "g")

    chunk = 2 * own
    mine = wrs[0:1, pl.ds(pl.multiple_of(mx * chunk, 128), chunk)]
    for f in range(2):
        wr_out[f : f + 1, :] = mine[:, f * own : (f + 1) * own]

    arrived(c2, s_c2, r_c2, "g")
    grid = c2[0]
    for n in range(1, CORES * G):
        grid = grid + c2[n]
    image = at_stations(grid)
    change = image - project(image)

    arrived(s2, s_s2, r_s2, "g")
    table = jnp.concatenate([s2[n] for n in range(CORES * G)], axis=0)
    peak = jnp.max(table[:, 0:1], axis=0, keepdims=True)
    change = change / peak
    sub_t = iota((T, 128), 0)
    step_rows = jnp.zeros((T, 128), f32)
    step_lanes = jnp.zeros((1, 128), f32)
    for k in range(T):
        step_rows = jnp.where(sub_t == k, steps[k], step_rows)
        step_lanes = jnp.where(lane == k, steps[k], step_lanes)
    moved = weight * (residual - step_rows[:, 0:1] * change)
    data = 0.5 * jnp.sum(moved * moved, axis=1, keepdims=True)
    data = jnp.sum(jnp.where(iota((T, 128), 1) == sub_t, data, 0.0), axis=0, keepdims=True)
    tau = step_lanes * (table[:, 1:2] / peak)
    energy = table[:, 6:7] * tau
    for n in (5, 4, 3):
        energy = (energy + table[:, n : n + 1]) * tau
    energy = energy + table[:, 2:3]
    energy = 0.5 * jnp.sum(energy, axis=0, keepdims=True)
    values = (data + coupling * energy) / (2 * total_stations)
    tv_out[...] = values[:, 0:T]

    for one in pending:
        one.wait_send()


def deliver(*refs):
    moves = [pltpu.make_async_copy(refs[n], refs[4 + n], refs[8].at[n]) for n in range(4)]
    for one in moves:
        one.start()
    for one in moves:
        one.wait()


def body(G, C, density, susceptibility, station_cell, station_line, observed, data_weight, trial_steps):
    R, W, K = density.shape
    own = station_cell.shape[1]
    NX, NY = R * G, W * C
    V = 2 * NY
    xp = 128 // V
    Q = NX // xp
    N = (NX + 8) * V
    ST = 2 * own * G
    T = trial_steps.shape[0]
    vmem = pl.BlockSpec(memory_space=pltpu.VMEM)
    dma = pltpu.SemaphoreType.DMA
    Z = C // CORES
    scratch = [
        pltpu.VMEM((R, W, K), f32),
        pltpu.VMEM((R, W, K), f32),
        pltpu.SMEM((T,), f32),
        dma((7,)),
        pltpu.VMEM((2, 2 * K, N), bf16),
        pltpu.VMEM((2, 2 * (W + 1) * 16, N), bf16),
        pltpu.VMEM((2, W + 1, 2, NX + 24, 128), f32),
        pltpu.VMEM((2, Q + 16, 128), f32),
        pltpu.VMEM((G, 2, own), jnp.int32),
        pltpu.VMEM((G, 2, own), jnp.int32),
        pltpu.VMEM((G, 2, own), f32),
        pltpu.VMEM((G, 2, own), f32),
        pltpu.VMEM((128, ST), bf16),
        pltpu.VMEM((Q, ST), f32),
        pltpu.VMEM((2 * HIGH, ST), f32),
        pltpu.VMEM((LOW, ST), bf16),
        pltpu.VMEM((1, ST), f32),
        pltpu.VMEM((Z, Q, 128), f32),
        pltpu.VMEM((CORES * G, Q, 128), f32),
        pltpu.VMEM((Z, Q, 128), f32),
        pltpu.VMEM((CORES * G, Q, 128), f32),
        pltpu.VMEM((Z, 8, 128), f32),
        pltpu.VMEM((CORES * G, -(-Z // 8) * 8, 128), f32),
        pltpu.VMEM((2, W + 2, 24, K), f32),
        pltpu.VMEM((6, 2, 8, K), f32),
        pltpu.VMEM((6, 2, 8, K), f32),
        pltpu.VMEM((2, 2, 8, K), f32),
        pltpu.VMEM((2, 2, 8, K), f32),
        pltpu.VMEM((2, W + 1, 16, K), f32),
        pltpu.VMEM((2, W + 1, 24, K), f32),
        dma((4, G)), dma((4, G)),
        dma((6,)), dma((6,)),
        dma((2,)), dma((2,)),
        dma((Z,)), dma((Z,)),
        dma((CORES * G,)), dma((CORES * G,)),
        dma((Z,)), dma((Z,)),
        dma((CORES * G,)), dma((CORES * G,)),
        dma((Z,)), dma((Z,)),
        dma((CORES * G,)), dma((CORES * G,)),
    ]
    out = pl.pallas_call(
        functools.partial(kernel, G, C),
        out_shape=(
            pltpu.VMEM((2, R, W, K), f32),
            pltpu.VMEM((2, R, W, K), f32),
            pltpu.VMEM((2, own), f32),
            pltpu.VMEM((1, T), f32),
        ),
        in_specs=[pl.BlockSpec(memory_space=pltpu.HBM)] * 7,
        out_specs=(vmem,) * 4,
        scratch_shapes=scratch,
        compiler_params=pltpu.CompilerParams(
            collective_id=0, has_side_effects=True, vmem_limit_bytes=60 * 1024 * 1024
        ),
    )(density, susceptibility, station_cell, station_line, observed, data_weight, trial_steps)
    out = pl.pallas_call(
        deliver,
        out_shape=tuple(jax.ShapeDtypeStruct(x.shape, x.dtype) for x in out),
        in_specs=[vmem] * 4,
        out_specs=(pl.BlockSpec(memory_space=pltpu.HBM),) * 4,
        scratch_shapes=[dma((4,))],
        compiler_params=pltpu.CompilerParams(vmem_limit_bytes=1024 * 1024),
    )(*out)
    return out[0], out[1], out[2], out[3].reshape(-1)


def solution(mesh):
    placed = (
        P("gx", "gy", None),
        P("gx", "gy", None),
        P(None, "gx"),
        P(None, "gx"),
        P(None, "gx"),
        P(None, "gx"),
        P(),
    )
    return jax.shard_map(
        functools.partial(body, mesh.shape["gx"], mesh.shape["gy"]),
        mesh=mesh,
        in_specs=placed,
        out_specs=(P(None, "gx", "gy", None), P(None, "gx", "gy", None), P(None, "gx"), P()),
        check_vma=False,
    )
```

```python
import functools

import jax
import jax.numpy as jnp
from jax import lax
from jax.experimental import pallas as pl
from jax.experimental.pallas import tpu as pltpu
from jax.sharding import PartitionSpec as P

LINES = 256
LOW = 32
CORES = 2
HIGH = LINES // LOW

cell_depth = 2.0
lift = 1.0
coupling_scale = 0.05

MESH = pl.DeviceIdType.MESH
f32 = jnp.float32
bf16 = jnp.bfloat16
NN = (((1,), (0,)), ((), ()))
NT = (((1,), (1,)), ((), ()))


def iota(shape, dim):
    return lax.broadcasted_iota(jnp.int32, shape, dim)


def split2(x):
    high = x.astype(bf16)
    return high, (x - high.astype(f32)).astype(bf16)


def split3(x):
    high = x.astype(bf16)
    rest = x - high.astype(f32)
    middle = rest.astype(bf16)
    return high, middle, (rest - middle.astype(f32)).astype(bf16)


def thirds(x):
    n = x.shape[0] // 3
    return x[:n] + x[n : 2 * n] + x[2 * n :]


def cross(a, b):
    return (a[1] * b[2] - a[2] * b[1], a[2] * b[0] - a[0] * b[2], a[0] * b[1] - a[1] * b[0])


def dot3(a, b):
    return a[0] * b[0] + a[1] * b[1] + a[2] * b[2]


def total(x):
    return jnp.sum(jnp.sum(x, axis=0, keepdims=True), axis=1, keepdims=True)


def largest(x):
    return jnp.max(jnp.max(x, axis=0, keepdims=True), axis=1, keepdims=True)


def kernel(
    G, C, den_in, sus_in, cell_in, line_in, obs_in, wgt_in, steps_in,
    dg_out, cf_out, wr_out, tv_out,
    den, sus, steps, s_in, E2, RS, F, A, cellb, lineb, obsb, wgtb, OY, OX, OHI, OLO, wrs,
    b1, b2, c1, c2, s1, s2, M, SH, RH, CH, CR, CFX, GE,
    s_st, r_st, s_h, r_h, s_c, r_c, s_b1, r_b1, s_b2, r_b2, s_c1, r_c1, s_c2, r_c2, s_s1, r_s1, s_s2, r_s2,
):
    R, W, K = den.shape
    own = cell_in.shape[1]
    NX, NY = R * G, W * C
    V = 2 * NY
    xp = 128 // V
    Q = NX // xp
    N = E2.shape[2]
    nch = N // 128
    ST = 2 * own * G
    T = steps.shape[0]
    mx = lax.axis_index("gx")
    my = lax.axis_index("gy")
    x0 = mx * R
    y0 = my * W
    total_stations = own * G
    coupling = coupling_scale * total_stations / (NX * NY * K)

    def at(dx, dy):
        return (lax.rem(mx + dx + G, G), lax.rem(my + dy + C, C))

    Z = C // CORES
    chip, core = my // CORES, lax.rem(my, CORES)
    zcast = [at(0, CORES * d) for d in range(1, Z)]
    xcast = [at(d, 0) for d in range(1, G)]
    gcast = xcast + [
        (lax.rem(mx + d, G), chip * CORES + lax.rem(core + e, CORES)) for e in range(1, CORES) for d in range(G)
    ]
    groups = {
        "z": (zcast, chip, [lax.rem(chip + d, Z) for d in range(1, Z)]),
        "x": (xcast, mx, [lax.rem(mx + d, G) for d in range(1, G)]),
        "g": (
            gcast,
            mx * CORES + core,
            [lax.rem(mx + d, G) * CORES + core for d in range(1, G)]
            + [
                lax.rem(mx + d, G) * CORES + lax.rem(core + e, CORES)
                for e in range(1, CORES)
                for d in range(G)
            ],
        ),
    }
    slot = mx * CORES + core
    barrier = pltpu.get_barrier_semaphore()
    partners = zcast + gcast + [at(0, 1), at(0, -1), at(1, -1), at(-1, 1)]
    for where in partners:
        pl.semaphore_signal(barrier, inc=1, device_id=where, device_id_type=MESH)

    loads = [
        pltpu.make_async_copy(src, dst, s_in.at[n])
        for n, (src, dst) in enumerate(
            (
                (den_in, den),
                (sus_in, sus),
                (cell_in, cellb.at[mx]),
                (line_in, lineb.at[mx]),
                (obs_in, obsb.at[mx]),
                (wgt_in, wgtb.at[mx]),
                (steps_in, steps),
            )
        )
    ]
    for one in loads:
        one.start()

    lane = iota((1, 128), 1)

    h_col = (iota((K, 128), 0).astype(f32) + 0.5) * cell_depth + lift
    h2 = h_col * h_col

    def table_turn(n, carry):
        gap_x = (n * xp + lane // V - 8 - x0).astype(f32)
        gap_y = (lane % V - 4 - y0).astype(f32)
        r2 = (gap_x * gap_x + gap_y * gap_y) + h2
        inverse = lax.rsqrt(r2)
        inverse2 = inverse * inverse
        cube = inverse2 * inverse
        both = (h_col * cube, (3.0 * h2 - r2) * cube * inverse2)
        spot = pl.ds(pl.multiple_of(n * 128, 128), 128)
        for f in range(2):
            high, low = split2(both[f])
            E2[f, 0:K, spot] = high
            E2[f, K : 2 * K, spot] = low
        return carry

    lax.fori_loop(0, nch, table_turn, 0)

    in_y = (lane % V) < NY

    def forward(columns, f):
        x = jnp.concatenate(columns, axis=0)
        high, low = split2(x)
        left = jnp.concatenate(
            [jnp.concatenate([high, high], axis=1), jnp.concatenate([low, low], axis=1)], axis=0
        )
        t = lax.dot_general(left, E2[f], NN, preferred_element_type=f32)
        t = t[: R * W] + t[R * W :]
        t2 = sum(pltpu.roll(t[j * R : (j + 1) * R], N - (4 - j), 1) for j in range(W))
        shifted = [t2] + [pltpu.roll(t2, N - c * V, 1) for c in range(1, xp)]
        sub = iota((R, NX * V), 0)
        acc = jnp.zeros((R, NX * V), f32)
        for i in range(R):
            s = 8 - i
            first = (s // xp) * 128
            acc = jnp.where(sub == i, shifted[s % xp][:, first : first + NX * V], acc)
        row = jnp.sum(acc, axis=0, keepdims=True)
        grid = jnp.concatenate([row[:, q * 128 : (q + 1) * 128] for q in range(Q)], axis=0)
        grid = jnp.where(in_y, grid, 0.0)
        return grid[: Q // 2] + pltpu.roll(grid[Q // 2 :], NY, 1)

    for one in loads[:2]:
        one.wait()
    models = (den, sus)
    own_columns = [[models[f][:, j, :] for j in range(W)] for f in range(2)]
    def copy(src, dst, ssem, rsem, where):
        return pltpu.make_async_remote_copy(
            src_ref=src, dst_ref=dst, send_sem=ssem, recv_sem=rsem,
            device_id=where, device_id_type=MESH,
        )

    pending = []

    def share(buf, ssem, rsem, group):
        targets, mine, _ = groups[group]
        for d, where in enumerate(targets):
            one = copy(buf.at[mine], buf.at[mine], ssem.at[d], rsem.at[mine], where)
            one.start()
            pending.append(one)

    def arrived(buf, ssem, rsem, group):
        targets, _, sources = groups[group]
        for src in sources:
            copy(buf.at[src], buf.at[src], ssem.at[0], rsem.at[src], targets[0]).wait_recv()

    b1[0, chip] = forward(own_columns[0], 0)
    pl.semaphore_wait(barrier, len(partners))
    share(b1.at[0], s_b1.at[0], r_b1.at[0], "z")
    b1[1, chip] = forward(own_columns[1], 1)
    share(b1.at[1], s_b1.at[1], r_b1.at[1], "z")
    for one in loads[2:]:
        one.wait()
    station_bufs = (cellb, lineb, obsb, wgtb)
    for n, buf in enumerate(station_bufs):
        share(buf, s_st.at[n], r_st.at[n], "x")
    M[...] = jnp.zeros(M.shape, f32)
    F[...] = jnp.zeros(F.shape, f32)
    A[...] = jnp.zeros(A.shape, f32)
    CFX[...] = jnp.zeros(CFX.shape, f32)
    SH[...] = jnp.zeros(SH.shape, f32)
    CH[...] = jnp.zeros(CH.shape, f32)
    s2[slot] = jnp.zeros(s2.shape[1:], f32)
    for f in range(2):
        for j in range(W):
            M[f, j + 1, 1 : R + 1, :] = own_columns[f][j]
        SH[0, f, 0:W, :] = models[f][R - 1]
        SH[1, f, 0:W, :] = models[f][0]
        SH[2, f, 0:R, :] = own_columns[f][W - 1]
        SH[3, f, 0:R, :] = own_columns[f][0]
        SH[4, f, 0:1, :] = models[f][R - 1, 0:1, :]
        SH[5, f, 0:1, :] = models[f][0, W - 1 : W, :]
    halo_targets = [at(1, 0), at(-1, 0), at(0, 1), at(0, -1), at(1, -1), at(-1, 1)]
    halos = []
    for n, where in enumerate(halo_targets):
        one = copy(SH.at[n], RH.at[n], s_h.at[n], r_h.at[n], where)
        one.start()
        halos.append(one)
        pending.append(one)

    for n, buf in enumerate(station_bufs):
        arrived(buf, s_st.at[n], r_st.at[n], "x")

    def spread_out(buf):
        return jnp.concatenate([buf[g, f : f + 1, :] for g in range(G) for f in range(2)], axis=1)

    field_of = (iota((1, ST), 1) // own) % 2
    cells = spread_out(cellb)
    lines = spread_out(lineb)
    observed = spread_out(obsb)
    weight = spread_out(wgtb)
    at_x = cells // NY
    at_y = cells - at_x * NY
    key_lane = (at_x % xp) * V + (at_x // (NX // 2)) * NY + at_y
    key_row = field_of * (Q // 2) + (at_x // xp) % (Q // 2)
    OY[...] = jnp.where(iota((128, ST), 0) == key_lane, 1.0, 0.0).astype(bf16)
    OX[...] = jnp.where(iota((Q, ST), 0) == key_row, 1.0, 0.0)
    OHI[...] = jnp.where(iota((2 * HIGH, ST), 0) == field_of * HIGH + lines // LOW, 1.0, 0.0)
    OLO[...] = jnp.where(iota((LOW, ST), 0) == lines % LOW, 1.0, 0.0).astype(bf16)
    counts = lax.dot_general(OHI[...].astype(bf16), OLO[...], NT, preferred_element_type=f32)
    per_line = 1.0 / jnp.maximum(counts, 1.0)

    def by_row(mask, v):
        return jnp.concatenate([(mask * p.astype(f32)).astype(bf16) for p in split3(v)], axis=0)

    def project(v):
        sums = lax.dot_general(by_row(OHI[...], v), OLO[...], NT, preferred_element_type=f32)
        means = thirds(sums) * per_line
        parts = jnp.concatenate(split3(means), axis=0)
        back = lax.dot_general(parts, OLO[...], NN, preferred_element_type=f32)
        return jnp.sum(thirds(back) * OHI[...], axis=0, keepdims=True)

    def at_stations(grid):
        parts = jnp.concatenate(split3(grid), axis=0)
        back = lax.dot_general(parts, OY[...], NN, preferred_element_type=f32)
        return jnp.sum(thirds(back) * OX[...], axis=0, keepdims=True)

    def pass_on(first, sends1, recvs1, second, sends2, recvs2, f):
        arrived(first.at[f], sends1.at[f], recvs1.at[f], "z")
        partial = first[f, 0]
        for n in range(1, Z):
            partial = partial + first[f, n]
        second[f, slot] = partial
        share(second.at[f], sends2.at[f], recvs2.at[f], "g")

    def gathered(buf, sends, recvs):
        halves = []
        for f in range(2):
            arrived(buf.at[f], sends.at[f], recvs.at[f], "g")
            grid = buf[f, 0]
            for n in range(1, CORES * G):
                grid = grid + buf[f, n]
            halves.append(grid)
        return jnp.concatenate(halves, axis=0)

    for f in range(2):
        pass_on(b1, s_b1, r_b1, b2, s_b2, r_b2, f)

    for one in halos:
        one.wait_recv()
    for f in range(2):
        for j in range(W):
            M[f, j + 1, 0:1, :] = RH[0, f, j : j + 1, :]
            M[f, j + 1, R + 1 : R + 2, :] = RH[1, f, j : j + 1, :]
        M[f, 0, 1 : R + 1, :] = RH[2, f, 0:R, :]
        M[f, W + 1, 1 : R + 1, :] = RH[3, f, 0:R, :]
        M[f, W + 1, 0:1, :] = RH[4, f, 0:1, :]
        M[f, 0, R + 1 : R + 2, :] = RH[5, f, 0:1, :]
    mask_z = (iota((1, K), 1) < K - 1).astype(f32)

    def diffs(ref, f, c, row, count, global_x, global_y):
        base = ref[f, c, row : row + count, :]
        up = ref[f, c, row + 1 : row + 1 + count, :]
        right = ref[f, c + 1, row : row + count, :]
        keep_x = (global_x < NX - 1).astype(f32)
        keep_y = (global_y < NY - 1).astype(f32)
        return (
            (up - base) * keep_x,
            (right - base) * keep_y,
            (pltpu.roll(base, K - 1, 1) - base) * mask_z,
        )

    gx_rim = x0 - 1 + iota((16, K), 0)
    before = [None, None]
    for c in range(W + 1):
        gy_rim = y0 - 1 + c + jnp.zeros((16, K), jnp.int32)
        a = diffs(M, 0, c, 0, 16, gx_rim, gy_rim)
        b = diffs(M, 1, c, 0, 16, gx_rim, gy_rim)
        valid = ((gx_rim >= 0) & (gy_rim >= 0)).astype(f32)
        t = tuple(part * valid for part in cross(a, b))
        keep_x = (gx_rim < NX - 1).astype(f32)
        keep_y = (gy_rim < NY - 1).astype(f32)
        for f, force in enumerate((cross(b, t), cross(t, a))):
            fx, fy, fz = force[0] * keep_x, force[1] * keep_y, force[2] * mask_z
            if c > 0:
                d = before[f] - fy - fx + pltpu.roll(fz, 1, 1) - fz
                result = pltpu.roll(d, 15, 0)[0:R] + fx[0:R]
                CFX[f, c - 1, 0:R, :] = result
                cf_out[f, :, c - 1, :] = result
                CH[0, f, c - 1 : c, :] = result[0:1]
                if c == 1:
                    CH[1, f, 0:R, :] = result
            before[f] = fy
    force_halos = []
    for n, where in enumerate((at(-1, 0), at(0, -1))):
        one = copy(CH.at[n], CR.at[n], s_c.at[n], r_c.at[n], where)
        one.start()
        force_halos.append(one)
        pending.append(one)

    misfit = at_stations(gathered(b2, s_b2, r_b2)) - observed
    residual = misfit - project(misfit)
    weighted = weight * residual
    wrs[...] = weighted
    source = weight * weighted
    source = source - project(source)
    S = thirds(
        lax.dot_general(by_row(OX[...], source), OY[...], NT, preferred_element_type=f32)
    )

    for one in force_halos:
        one.wait_recv()
    for f in range(2):
        for j in range(W):
            CFX[f, j, R : R + 1, :] = CR[0, f, j : j + 1, :]
        CFX[f, W, 0:R, :] = CR[1, f, 0:R, :]

    for f in range(2):
        half_f = S[f * (Q // 2) : (f + 1) * (Q // 2)]
        A[f, 8 : 8 + Q // 2, :] = jnp.where(in_y, half_f, 0.0)
        A[f, 8 + Q // 2 : 8 + Q, :] = jnp.where(in_y, pltpu.roll(half_f, 128 - NY, 1), 0.0)
        for j in range(W + 1):
            now = A[f, 7 : 7 + Q + 8, :]
            later = A[f, 8 : 8 + Q + 8, :]
            for c in range(xp):
                turn = (4 - j + 128 - c * V) % 128
                first = now if turn == 0 else pltpu.roll(now, turn, 1)
                second = later if turn == 0 else pltpu.roll(later, turn, 1)
                value = first if c == 0 else jnp.where(lane < 128 - c * V, first, second)
                high, low = split2(value)
                rows = pl.ds(8 - xp + c, Q + 8, stride=xp) if xp > 1 else pl.ds(7, Q + 8)
                F[f, j, 0, rows, :] = high.astype(f32)
                F[f, j, 1, rows, :] = low.astype(f32)
        for j in range(W + 1):
            for h in range(2):
                for n in range(nch):
                    RS[f, (h * (W + 1) + j) * 16 : (h * (W + 1) + j + 1) * 16, n * 128 : (n + 1) * 128] = F[
                        f, j, h, n * xp : n * xp + 16, :
                    ].astype(bf16)
        D = lax.dot_general(RS[f], E2[f], NT, preferred_element_type=f32)
        half = (W + 1) * 16
        D = D[:half] + D[half:]
        D = D[:, :K] + D[:, K:]
        for j in range(W + 1):
            piece = D[j * 16 : (j + 1) * 16]
            GE[f, j, 0:16, :] = piece + coupling * CFX[f, j]
            if j < W:
                dg_out[f, :, j, :] = piece[0:R]
        c1[f, chip] = forward([GE[f, j, 0:R, :] for j in range(W)], f)
        share(c1.at[f], s_c1.at[f], r_c1.at[f], "z")

    g_columns = [[GE[f, j, 0:R, :] for j in range(W)] for f in range(2)]

    sub16 = iota((16, K), 0)
    own_peak = functools.reduce(
        jnp.maximum, [jnp.abs(g_columns[f][j]) for f in range(2) for j in range(W)]
    )
    rim_peak = functools.reduce(
        jnp.maximum,
        [jnp.where(sub16 <= R, jnp.abs(GE[f, j, 0:16, :]), 0.0) for f in range(2) for j in range(W + 1)],
    )
    own_peak = largest(own_peak) + 1e-06
    scale = largest(rim_peak) + 1e-06
    for f in range(2):
        for j in range(W + 1):
            GE[f, j, 0:16, :] = GE[f, j, 0:16, :] / scale
    gx_own = x0 + iota((R, K), 0)
    powers = [jnp.zeros((R, K), f32) for _ in range(5)]
    for j in range(W):
        gy_own = y0 + j + jnp.zeros((R, K), jnp.int32)
        a = diffs(M, 0, j + 1, 1, R, gx_own, gy_own)
        b = diffs(M, 1, j + 1, 1, R, gx_own, gy_own)
        da = diffs(GE, 0, j, 0, R, gx_own, gy_own)
        db = diffs(GE, 1, j, 0, R, gx_own, gy_own)
        u = cross(a, b)
        v = tuple(p + q for p, q in zip(cross(da, b), cross(a, db)))
        w = cross(da, db)
        powers[0] += dot3(u, u)
        powers[1] -= 2.0 * dot3(u, v)
        powers[2] += dot3(v, v) + 2.0 * dot3(u, w)
        powers[3] -= 2.0 * dot3(v, w)
        powers[4] += dot3(w, w)
    scalars = [own_peak, scale] + [total(p) for p in powers]
    lane8 = iota((8, 128), 1)
    message = jnp.zeros((8, 128), f32)
    for n, value in enumerate(scalars):
        message = jnp.where(lane8 == n, value, message)
    s1[chip] = message
    share(s1, s_s1, r_s1, "z")

    for f in range(2):
        pass_on(c1, s_c1, r_c1, c2, s_c2, r_c2, f)
    arrived(s1, s_s1, r_s1, "z")
    s2[slot, 0:Z, :] = jnp.concatenate([s1[n, 0:1, :] for n in range(Z)], axis=0)
    share(s2, s_s2, r_s2, "g")

    chunk = 2 * own
    mine = wrs[0:1, pl.ds(pl.multiple_of(mx * chunk, 128), chunk)]
    for f in range(2):
        wr_out[f : f + 1, :] = mine[:, f * own : (f + 1) * own]

    image = at_stations(gathered(c2, s_c2, r_c2))
    change = image - project(image)

    arrived(s2, s_s2, r_s2, "g")
    table = jnp.concatenate([s2[n] for n in range(CORES * G)], axis=0)
    peak = jnp.max(table[:, 0:1], axis=0, keepdims=True)
    change = change / peak
    sub_t = iota((T, 128), 0)
    step_rows = jnp.zeros((T, 128), f32)
    step_lanes = jnp.zeros((1, 128), f32)
    for k in range(T):
        step_rows = jnp.where(sub_t == k, steps[k], step_rows)
        step_lanes = jnp.where(lane == k, steps[k], step_lanes)
    moved = weight * (residual - step_rows[:, 0:1] * change)
    data = 0.5 * jnp.sum(moved * moved, axis=1, keepdims=True)
    data = jnp.sum(jnp.where(iota((T, 128), 1) == sub_t, data, 0.0), axis=0, keepdims=True)
    tau = step_lanes * (table[:, 1:2] / peak)
    energy = table[:, 6:7] * tau
    for n in (5, 4, 3):
        energy = (energy + table[:, n : n + 1]) * tau
    energy = energy + table[:, 2:3]
    energy = 0.5 * jnp.sum(energy, axis=0, keepdims=True)
    values = (data + coupling * energy) / (2 * total_stations)
    tv_out[...] = values[:, 0:T]

    for one in pending:
        one.wait_send()


def deliver(*refs):
    moves = [pltpu.make_async_copy(refs[n], refs[4 + n], refs[8].at[n]) for n in range(4)]
    for one in moves:
        one.start()
    for one in moves:
        one.wait()


def body(G, C, density, susceptibility, station_cell, station_line, observed, data_weight, trial_steps):
    R, W, K = density.shape
    own = station_cell.shape[1]
    NX, NY = R * G, W * C
    V = 2 * NY
    xp = 128 // V
    Q = NX // xp
    N = (NX + 8) * V
    ST = 2 * own * G
    T = trial_steps.shape[0]
    vmem = pl.BlockSpec(memory_space=pltpu.VMEM)
    dma = pltpu.SemaphoreType.DMA
    Z = C // CORES
    scratch = [
        pltpu.VMEM((R, W, K), f32),
        pltpu.VMEM((R, W, K), f32),
        pltpu.SMEM((T,), f32),
        dma((7,)),
        pltpu.VMEM((2, 2 * K, N), bf16),
        pltpu.VMEM((2, 2 * (W + 1) * 16, N), bf16),
        pltpu.VMEM((2, W + 1, 2, NX + 24, 128), f32),
        pltpu.VMEM((2, Q + 16, 128), f32),
        pltpu.VMEM((G, 2, own), jnp.int32),
        pltpu.VMEM((G, 2, own), jnp.int32),
        pltpu.VMEM((G, 2, own), f32),
        pltpu.VMEM((G, 2, own), f32),
        pltpu.VMEM((128, ST), bf16),
        pltpu.VMEM((Q, ST), f32),
        pltpu.VMEM((2 * HIGH, ST), f32),
        pltpu.VMEM((LOW, ST), bf16),
        pltpu.VMEM((1, ST), f32),
        pltpu.VMEM((2, Z, Q // 2, 128), f32),
        pltpu.VMEM((2, CORES * G, Q // 2, 128), f32),
        pltpu.VMEM((2, Z, Q // 2, 128), f32),
        pltpu.VMEM((2, CORES * G, Q // 2, 128), f32),
        pltpu.VMEM((Z, 8, 128), f32),
        pltpu.VMEM((CORES * G, -(-Z // 8) * 8, 128), f32),
        pltpu.VMEM((2, W + 2, 24, K), f32),
        pltpu.VMEM((6, 2, 8, K), f32),
        pltpu.VMEM((6, 2, 8, K), f32),
        pltpu.VMEM((2, 2, 8, K), f32),
        pltpu.VMEM((2, 2, 8, K), f32),
        pltpu.VMEM((2, W + 1, 16, K), f32),
        pltpu.VMEM((2, W + 1, 24, K), f32),
        dma((4, G)), dma((4, G)),
        dma((6,)), dma((6,)),
        dma((2,)), dma((2,)),
        dma((2, Z)), dma((2, Z)),
        dma((2, CORES * G)), dma((2, CORES * G)),
        dma((2, Z)), dma((2, Z)),
        dma((2, CORES * G)), dma((2, CORES * G)),
        dma((Z,)), dma((Z,)),
        dma((CORES * G,)), dma((CORES * G,)),
    ]
    out = pl.pallas_call(
        functools.partial(kernel, G, C),
        out_shape=(
            pltpu.VMEM((2, R, W, K), f32),
            pltpu.VMEM((2, R, W, K), f32),
            pltpu.VMEM((2, own), f32),
            pltpu.VMEM((1, T), f32),
        ),
        in_specs=[pl.BlockSpec(memory_space=pltpu.HBM)] * 7,
        out_specs=(vmem,) * 4,
        scratch_shapes=scratch,
        compiler_params=pltpu.CompilerParams(
            collective_id=0, has_side_effects=True, vmem_limit_bytes=60 * 1024 * 1024
        ),
    )(density, susceptibility, station_cell, station_line, observed, data_weight, trial_steps)
    out = pl.pallas_call(
        deliver,
        out_shape=tuple(jax.ShapeDtypeStruct(x.shape, x.dtype) for x in out),
        in_specs=[vmem] * 4,
        out_specs=(pl.BlockSpec(memory_space=pltpu.HBM),) * 4,
        scratch_shapes=[dma((4,))],
        compiler_params=pltpu.CompilerParams(vmem_limit_bytes=1024 * 1024),
    )(*out)
    return out[0], out[1], out[2], out[3].reshape(-1)


def solution(mesh):
    placed = (
        P("gx", "gy", None),
        P("gx", "gy", None),
        P(None, "gx"),
        P(None, "gx"),
        P(None, "gx"),
        P(None, "gx"),
        P(),
    )
    return jax.shard_map(
        functools.partial(body, mesh.shape["gx"], mesh.shape["gy"]),
        mesh=mesh,
        in_specs=placed,
        out_specs=(P(None, "gx", "gy", None), P(None, "gx", "gy", None), P(None, "gx"), P()),
        check_vma=False,
    )
```

```python
import functools

import jax
import jax.numpy as jnp
from jax import lax
from jax.experimental import pallas as pl
from jax.experimental.pallas import tpu as pltpu
from jax.sharding import PartitionSpec as P

LINES = 256
LOW = 32
CORES = 2
HIGH = LINES // LOW

cell_depth = 2.0
lift = 1.0
coupling_scale = 0.05

MESH = pl.DeviceIdType.MESH
f32 = jnp.float32
bf16 = jnp.bfloat16
NN = (((1,), (0,)), ((), ()))
NT = (((1,), (1,)), ((), ()))


def iota(shape, dim):
    return lax.broadcasted_iota(jnp.int32, shape, dim)


def split2(x):
    high = x.astype(bf16)
    return high, (x - high.astype(f32)).astype(bf16)


def split3(x):
    high = x.astype(bf16)
    rest = x - high.astype(f32)
    middle = rest.astype(bf16)
    return high, middle, (rest - middle.astype(f32)).astype(bf16)


def thirds(x):
    n = x.shape[0] // 3
    return x[:n] + x[n : 2 * n] + x[2 * n :]


def cross(a, b):
    return (a[1] * b[2] - a[2] * b[1], a[2] * b[0] - a[0] * b[2], a[0] * b[1] - a[1] * b[0])


def dot3(a, b):
    return a[0] * b[0] + a[1] * b[1] + a[2] * b[2]


def total(x):
    return jnp.sum(jnp.sum(x, axis=0, keepdims=True), axis=1, keepdims=True)


def largest(x):
    return jnp.max(jnp.max(x, axis=0, keepdims=True), axis=1, keepdims=True)


def kernel(
    G, C, den_in, sus_in, cell_in, line_in, obs_in, wgt_in, steps_in,
    dg_out, cf_out, wr_out, tv_out,
    den, sus, steps, s_in, E2, RS, F, A, st, cellb, lineb, obsb, wgtb, OY, OX, OHI, OLO, wrs,
    b1, b2, c1, c2, s1, s2, M, SH, RH, CH, CR, CFX, GE,
    s_st, r_st, s_h, r_h, s_c, r_c, s_b1, r_b1, s_b2, r_b2, s_c1, r_c1, s_c2, r_c2, s_s1, r_s1, s_s2, r_s2,
):
    R, W, K = den.shape
    own = cell_in.shape[1]
    NX, NY = R * G, W * C
    V = 2 * NY
    xp = 128 // V
    Q = NX // xp
    N = E2.shape[2]
    nch = N // 128
    ST = 2 * own * G
    T = steps.shape[0]
    mx = lax.axis_index("gx")
    my = lax.axis_index("gy")
    x0 = mx * R
    y0 = my * W
    total_stations = own * G
    coupling = coupling_scale * total_stations / (NX * NY * K)

    def at(dx, dy):
        return (lax.rem(mx + dx + G, G), lax.rem(my + dy + C, C))

    Z = C // CORES
    chip, core = my // CORES, lax.rem(my, CORES)
    zcast = [at(0, CORES * d) for d in range(1, Z)]
    xcast = [at(d, 0) for d in range(1, G)]
    gcast = xcast + [
        (lax.rem(mx + d, G), chip * CORES + lax.rem(core + e, CORES)) for e in range(1, CORES) for d in range(G)
    ]
    groups = {
        "z": (zcast, chip, [lax.rem(chip + d, Z) for d in range(1, Z)]),
        "x": (xcast, mx, [lax.rem(mx + d, G) for d in range(1, G)]),
        "g": (
            gcast,
            mx * CORES + core,
            [lax.rem(mx + d, G) * CORES + core for d in range(1, G)]
            + [
                lax.rem(mx + d, G) * CORES + lax.rem(core + e, CORES)
                for e in range(1, CORES)
                for d in range(G)
            ],
        ),
    }
    slot = mx * CORES + core
    barrier = pltpu.get_barrier_semaphore()
    partners = zcast + gcast + [at(0, 1), at(0, -1), at(1, -1), at(-1, 1)]
    for where in partners:
        pl.semaphore_signal(barrier, inc=1, device_id=where, device_id_type=MESH)

    loads = [
        pltpu.make_async_copy(src, dst, s_in.at[n])
        for n, (src, dst) in enumerate(
            (
                (den_in, den),
                (sus_in, sus),
                (cell_in, cellb),
                (line_in, lineb),
                (obs_in, obsb),
                (wgt_in, wgtb),
                (steps_in, steps),
            )
        )
    ]
    for one in loads:
        one.start()

    lane = iota((1, 128), 1)

    h_col = (iota((K, 128), 0).astype(f32) + 0.5) * cell_depth + lift
    h2 = h_col * h_col

    def table_turn(n, carry):
        gap_x = (n * xp + lane // V - 8 - x0).astype(f32)
        gap_y = (lane % V - 4 - y0).astype(f32)
        r2 = (gap_x * gap_x + gap_y * gap_y) + h2
        inverse = lax.rsqrt(r2)
        inverse2 = inverse * inverse
        cube = inverse2 * inverse
        both = (h_col * cube, (3.0 * h2 - r2) * cube * inverse2)
        spot = pl.ds(pl.multiple_of(n * 128, 128), 128)
        for f in range(2):
            high, low = split2(both[f])
            E2[f, 0:K, spot] = high
            E2[f, K : 2 * K, spot] = low
        return carry

    lax.fori_loop(0, nch, table_turn, 0)

    in_y = (lane % V) < NY

    def forward(columns, f):
        x = jnp.concatenate(columns, axis=0)
        high, low = split2(x)
        left = jnp.concatenate(
            [jnp.concatenate([high, high], axis=1), jnp.concatenate([low, low], axis=1)], axis=0
        )
        t = lax.dot_general(left, E2[f], NN, preferred_element_type=f32)
        t = t[: R * W] + t[R * W :]
        t2 = sum(pltpu.roll(t[j * R : (j + 1) * R], N - (4 - j), 1) for j in range(W))
        shifted = [t2] + [pltpu.roll(t2, N - c * V, 1) for c in range(1, xp)]
        sub = iota((R, NX * V), 0)
        acc = jnp.zeros((R, NX * V), f32)
        for i in range(R):
            s = 8 - i
            first = (s // xp) * 128
            acc = jnp.where(sub == i, shifted[s % xp][:, first : first + NX * V], acc)
        row = jnp.sum(acc, axis=0, keepdims=True)
        grid = jnp.concatenate([row[:, q * 128 : (q + 1) * 128] for q in range(Q)], axis=0)
        grid = jnp.where(in_y, grid, 0.0)
        return grid if f == 0 else pltpu.roll(grid, NY, 1)

    for one in loads[:2]:
        one.wait()
    models = (den, sus)
    own_columns = [[models[f][:, j, :] for j in range(W)] for f in range(2)]
    b1[chip] = forward(own_columns[0], 0) + forward(own_columns[1], 1)

    pl.semaphore_wait(barrier, len(partners))

    def copy(src, dst, ssem, rsem, where):
        return pltpu.make_async_remote_copy(
            src_ref=src, dst_ref=dst, send_sem=ssem, recv_sem=rsem,
            device_id=where, device_id_type=MESH,
        )

    pending = []

    def share(buf, ssem, rsem, group):
        targets, mine, _ = groups[group]
        for d, where in enumerate(targets):
            one = copy(buf.at[mine], buf.at[mine], ssem.at[d], rsem.at[mine], where)
            one.start()
            pending.append(one)

    def arrived(buf, ssem, rsem, group):
        targets, _, sources = groups[group]
        for src in sources:
            copy(buf.at[src], buf.at[src], ssem.at[0], rsem.at[src], targets[0]).wait_recv()

    share(b1, s_b1, r_b1, "z")
    for one in loads[2:]:
        one.wait()
    for n, buf in enumerate((cellb, lineb, obsb, wgtb)):
        st[mx, 2 * n : 2 * n + 2, :] = buf[...].astype(f32)
    share(st, s_st, r_st, "x")
    M[...] = jnp.zeros(M.shape, f32)
    F[...] = jnp.zeros(F.shape, f32)
    A[...] = jnp.zeros(A.shape, f32)
    CFX[...] = jnp.zeros(CFX.shape, f32)
    SH[...] = jnp.zeros(SH.shape, f32)
    CH[...] = jnp.zeros(CH.shape, f32)
    s2[slot] = jnp.zeros(s2.shape[1:], f32)
    for f in range(2):
        for j in range(W):
            M[f, j + 1, 1 : R + 1, :] = own_columns[f][j]
        SH[0, f, 0:W, :] = models[f][R - 1]
        SH[1, f, 0:W, :] = models[f][0]
        SH[2, f, 0:R, :] = own_columns[f][W - 1]
        SH[3, f, 0:R, :] = own_columns[f][0]
        SH[4, f, 0:1, :] = models[f][R - 1, 0:1, :]
        SH[5, f, 0:1, :] = models[f][0, W - 1 : W, :]
    halo_targets = [at(1, 0), at(-1, 0), at(0, 1), at(0, -1), at(1, -1), at(-1, 1)]
    halos = []
    for n, where in enumerate(halo_targets):
        one = copy(SH.at[n], RH.at[n], s_h.at[n], r_h.at[n], where)
        one.start()
        halos.append(one)
        pending.append(one)

    arrived(b1, s_b1, r_b1, "z")
    partial = b1[0]
    for n in range(1, Z):
        partial = partial + b1[n]
    b2[slot] = partial
    share(b2, s_b2, r_b2, "g")

    arrived(st, s_st, r_st, "x")

    def spread_out(n):
        return jnp.concatenate(
            [st[g, 2 * n + f : 2 * n + f + 1, :] for g in range(G) for f in range(2)], axis=1
        )

    field_of = (iota((1, ST), 1) // own) % 2
    cells = spread_out(0).astype(jnp.int32)
    lines = spread_out(1).astype(jnp.int32)
    observed = spread_out(2)
    weight = spread_out(3)
    at_x = cells // NY
    at_y = cells - at_x * NY
    key_lane = (at_x % xp) * V + field_of * NY + at_y
    key_row = at_x // xp
    OY[...] = jnp.where(iota((128, ST), 0) == key_lane, 1.0, 0.0).astype(bf16)
    OX[...] = jnp.where(iota((Q, ST), 0) == key_row, 1.0, 0.0)
    OHI[...] = jnp.where(iota((2 * HIGH, ST), 0) == field_of * HIGH + lines // LOW, 1.0, 0.0)
    OLO[...] = jnp.where(iota((LOW, ST), 0) == lines % LOW, 1.0, 0.0).astype(bf16)
    counts = lax.dot_general(OHI[...].astype(bf16), OLO[...], NT, preferred_element_type=f32)
    per_line = 1.0 / jnp.maximum(counts, 1.0)

    def by_row(mask, v):
        return jnp.concatenate([(mask * p.astype(f32)).astype(bf16) for p in split3(v)], axis=0)

    def project(v):
        sums = lax.dot_general(by_row(OHI[...], v), OLO[...], NT, preferred_element_type=f32)
        means = thirds(sums) * per_line
        parts = jnp.concatenate(split3(means), axis=0)
        back = lax.dot_general(parts, OLO[...], NN, preferred_element_type=f32)
        return jnp.sum(thirds(back) * OHI[...], axis=0, keepdims=True)

    def at_stations(grid):
        parts = jnp.concatenate(split3(grid), axis=0)
        back = lax.dot_general(parts, OY[...], NN, preferred_element_type=f32)
        return jnp.sum(thirds(back) * OX[...], axis=0, keepdims=True)

    for one in halos:
        one.wait_recv()
    for f in range(2):
        for j in range(W):
            M[f, j + 1, 0:1, :] = RH[0, f, j : j + 1, :]
            M[f, j + 1, R + 1 : R + 2, :] = RH[1, f, j : j + 1, :]
        M[f, 0, 1 : R + 1, :] = RH[2, f, 0:R, :]
        M[f, W + 1, 1 : R + 1, :] = RH[3, f, 0:R, :]
        M[f, W + 1, 0:1, :] = RH[4, f, 0:1, :]
        M[f, 0, R + 1 : R + 2, :] = RH[5, f, 0:1, :]
    mask_z = (iota((1, K), 1) < K - 1).astype(f32)

    def diffs(ref, f, c, row, count, global_x, global_y):
        base = ref[f, c, row : row + count, :]
        up = ref[f, c, row + 1 : row + 1 + count, :]
        right = ref[f, c + 1, row : row + count, :]
        keep_x = (global_x < NX - 1).astype(f32)
        keep_y = (global_y < NY - 1).astype(f32)
        return (
            (up - base) * keep_x,
            (right - base) * keep_y,
            (pltpu.roll(base, K - 1, 1) - base) * mask_z,
        )

    gx_rim = x0 - 1 + iota((16, K), 0)
    before = [None, None]
    for c in range(W + 1):
        gy_rim = y0 - 1 + c + jnp.zeros((16, K), jnp.int32)
        a = diffs(M, 0, c, 0, 16, gx_rim, gy_rim)
        b = diffs(M, 1, c, 0, 16, gx_rim, gy_rim)
        valid = ((gx_rim >= 0) & (gy_rim >= 0)).astype(f32)
        t = tuple(part * valid for part in cross(a, b))
        keep_x = (gx_rim < NX - 1).astype(f32)
        keep_y = (gy_rim < NY - 1).astype(f32)
        for f, force in enumerate((cross(b, t), cross(t, a))):
            fx, fy, fz = force[0] * keep_x, force[1] * keep_y, force[2] * mask_z
            if c > 0:
                d = before[f] - fy - fx + pltpu.roll(fz, 1, 1) - fz
                result = pltpu.roll(d, 15, 0)[0:R] + fx[0:R]
                CFX[f, c - 1, 0:R, :] = result
                cf_out[f, :, c - 1, :] = result
                CH[0, f, c - 1 : c, :] = result[0:1]
                if c == 1:
                    CH[1, f, 0:R, :] = result
            before[f] = fy
    force_halos = []
    for n, where in enumerate((at(-1, 0), at(0, -1))):
        one = copy(CH.at[n], CR.at[n], s_c.at[n], r_c.at[n], where)
        one.start()
        force_halos.append(one)
        pending.append(one)

    arrived(b2, s_b2, r_b2, "g")
    grid = b2[0]
    for n in range(1, CORES * G):
        grid = grid + b2[n]

    misfit = at_stations(grid) - observed
    residual = misfit - project(misfit)
    weighted = weight * residual
    wrs[...] = weighted
    source = weight * weighted
    source = source - project(source)
    S = thirds(
        lax.dot_general(by_row(OX[...], source), OY[...], NT, preferred_element_type=f32)
    )

    for one in force_halos:
        one.wait_recv()
    for f in range(2):
        for j in range(W):
            CFX[f, j, R : R + 1, :] = CR[0, f, j : j + 1, :]
        CFX[f, W, 0:R, :] = CR[1, f, 0:R, :]

    for f in range(2):
        S_f = jnp.where(in_y, S if f == 0 else pltpu.roll(S, 128 - NY, 1), 0.0)
        A[f, 8 : 8 + Q, :] = S_f
        for j in range(W + 1):
            now = A[f, 7 : 7 + Q + 8, :]
            later = A[f, 8 : 8 + Q + 8, :]
            for c in range(xp):
                turn = (4 - j + 128 - c * V) % 128
                first = now if turn == 0 else pltpu.roll(now, turn, 1)
                second = later if turn == 0 else pltpu.roll(later, turn, 1)
                value = first if c == 0 else jnp.where(lane < 128 - c * V, first, second)
                high, low = split2(value)
                rows = pl.ds(8 - xp + c, Q + 8, stride=xp) if xp > 1 else pl.ds(7, Q + 8)
                F[f, j, 0, rows, :] = high.astype(f32)
                F[f, j, 1, rows, :] = low.astype(f32)
        for j in range(W + 1):
            for h in range(2):
                for n in range(nch):
                    RS[f, (h * (W + 1) + j) * 16 : (h * (W + 1) + j + 1) * 16, n * 128 : (n + 1) * 128] = F[
                        f, j, h, n * xp : n * xp + 16, :
                    ].astype(bf16)
        D = lax.dot_general(RS[f], E2[f], NT, preferred_element_type=f32)
        half = (W + 1) * 16
        D = D[:half] + D[half:]
        D = D[:, :K] + D[:, K:]
        for j in range(W + 1):
            piece = D[j * 16 : (j + 1) * 16]
            GE[f, j, 0:16, :] = piece + coupling * CFX[f, j]
            if j < W:
                dg_out[f, :, j, :] = piece[0:R]

    g_columns = [[GE[f, j, 0:R, :] for j in range(W)] for f in range(2)]
    c1[chip] = forward(g_columns[0], 0) + forward(g_columns[1], 1)
    share(c1, s_c1, r_c1, "z")

    sub16 = iota((16, K), 0)
    own_peak = functools.reduce(
        jnp.maximum, [jnp.abs(g_columns[f][j]) for f in range(2) for j in range(W)]
    )
    rim_peak = functools.reduce(
        jnp.maximum,
        [jnp.where(sub16 <= R, jnp.abs(GE[f, j, 0:16, :]), 0.0) for f in range(2) for j in range(W + 1)],
    )
    own_peak = largest(own_peak) + 1e-06
    scale = largest(rim_peak) + 1e-06
    for f in range(2):
        for j in range(W + 1):
            GE[f, j, 0:16, :] = GE[f, j, 0:16, :] / scale
    gx_own = x0 + iota((R, K), 0)
    powers = [jnp.zeros((R, K), f32) for _ in range(5)]
    for j in range(W):
        gy_own = y0 + j + jnp.zeros((R, K), jnp.int32)
        a = diffs(M, 0, j + 1, 1, R, gx_own, gy_own)
        b = diffs(M, 1, j + 1, 1, R, gx_own, gy_own)
        da = diffs(GE, 0, j, 0, R, gx_own, gy_own)
        db = diffs(GE, 1, j, 0, R, gx_own, gy_own)
        u = cross(a, b)
        v = tuple(p + q for p, q in zip(cross(da, b), cross(a, db)))
        w = cross(da, db)
        powers[0] += dot3(u, u)
        powers[1] -= 2.0 * dot3(u, v)
        powers[2] += dot3(v, v) + 2.0 * dot3(u, w)
        powers[3] -= 2.0 * dot3(v, w)
        powers[4] += dot3(w, w)
    scalars = [own_peak, scale] + [total(p) for p in powers]
    lane8 = iota((8, 128), 1)
    message = jnp.zeros((8, 128), f32)
    for n, value in enumerate(scalars):
        message = jnp.where(lane8 == n, value, message)
    s1[chip] = message
    share(s1, s_s1, r_s1, "z")

    arrived(c1, s_c1, r_c1, "z")
    partial = c1[0]
    for n in range(1, Z):
        partial = partial + c1[n]
    c2[slot] = partial
    share(c2, s_c2, r_c2, "g")
    arrived(s1, s_s1, r_s1, "z")
    s2[slot, 0:Z, :] = jnp.concatenate([s1[n, 0:1, :] for n in range(Z)], axis=0)
    share(s2, s_s2, r_s2, "g")

    chunk = 2 * own
    mine = wrs[0:1, pl.ds(pl.multiple_of(mx * chunk, 128), chunk)]
    for f in range(2):
        wr_out[f : f + 1, :] = mine[:, f * own : (f + 1) * own]

    arrived(c2, s_c2, r_c2, "g")
    grid = c2[0]
    for n in range(1, CORES * G):
        grid = grid + c2[n]
    image = at_stations(grid)
    change = image - project(image)

    arrived(s2, s_s2, r_s2, "g")
    table = jnp.concatenate([s2[n] for n in range(CORES * G)], axis=0)
    peak = jnp.max(table[:, 0:1], axis=0, keepdims=True)
    change = change / peak
    sub_t = iota((T, 128), 0)
    step_rows = jnp.zeros((T, 128), f32)
    step_lanes = jnp.zeros((1, 128), f32)
    for k in range(T):
        step_rows = jnp.where(sub_t == k, steps[k], step_rows)
        step_lanes = jnp.where(lane == k, steps[k], step_lanes)
    moved = weight * (residual - step_rows[:, 0:1] * change)
    data = 0.5 * jnp.sum(moved * moved, axis=1, keepdims=True)
    data = jnp.sum(jnp.where(iota((T, 128), 1) == sub_t, data, 0.0), axis=0, keepdims=True)
    tau = step_lanes * (table[:, 1:2] / peak)
    energy = table[:, 6:7] * tau
    for n in (5, 4, 3):
        energy = (energy + table[:, n : n + 1]) * tau
    energy = energy + table[:, 2:3]
    energy = 0.5 * jnp.sum(energy, axis=0, keepdims=True)
    values = (data + coupling * energy) / (2 * total_stations)
    tv_out[...] = values[:, 0:T]

    for one in pending:
        one.wait_send()


def deliver(*refs):
    moves = [pltpu.make_async_copy(refs[n], refs[4 + n], refs[8].at[n]) for n in range(4)]
    for one in moves:
        one.start()
    for one in moves:
        one.wait()


def body(G, C, density, susceptibility, station_cell, station_line, observed, data_weight, trial_steps):
    R, W, K = density.shape
    own = station_cell.shape[1]
    NX, NY = R * G, W * C
    V = 2 * NY
    xp = 128 // V
    Q = NX // xp
    N = (NX + 8) * V
    ST = 2 * own * G
    T = trial_steps.shape[0]
    vmem = pl.BlockSpec(memory_space=pltpu.VMEM)
    dma = pltpu.SemaphoreType.DMA
    Z = C // CORES
    scratch = [
        pltpu.VMEM((R, W, K), f32),
        pltpu.VMEM((R, W, K), f32),
        pltpu.SMEM((T,), f32),
        dma((7,)),
        pltpu.VMEM((2, 2 * K, N), bf16),
        pltpu.VMEM((2, 2 * (W + 1) * 16, N), bf16),
        pltpu.VMEM((2, W + 1, 2, NX + 24, 128), f32),
        pltpu.VMEM((2, Q + 16, 128), f32),
        pltpu.VMEM((G, 8, own), f32),
        pltpu.VMEM((2, own), jnp.int32),
        pltpu.VMEM((2, own), jnp.int32),
        pltpu.VMEM((2, own), f32),
        pltpu.VMEM((2, own), f32),
        pltpu.VMEM((128, ST), bf16),
        pltpu.VMEM((Q, ST), f32),
        pltpu.VMEM((2 * HIGH, ST), f32),
        pltpu.VMEM((LOW, ST), bf16),
        pltpu.VMEM((1, ST), f32),
        pltpu.VMEM((Z, Q, 128), f32),
        pltpu.VMEM((CORES * G, Q, 128), f32),
        pltpu.VMEM((Z, Q, 128), f32),
        pltpu.VMEM((CORES * G, Q, 128), f32),
        pltpu.VMEM((Z, 8, 128), f32),
        pltpu.VMEM((CORES * G, -(-Z // 8) * 8, 128), f32),
        pltpu.VMEM((2, W + 2, 24, K), f32),
        pltpu.VMEM((6, 2, 8, K), f32),
        pltpu.VMEM((6, 2, 8, K), f32),
        pltpu.VMEM((2, 2, 8, K), f32),
        pltpu.VMEM((2, 2, 8, K), f32),
        pltpu.VMEM((2, W + 1, 16, K), f32),
        pltpu.VMEM((2, W + 1, 24, K), f32),
        dma((G,)), dma((G,)),
        dma((6,)), dma((6,)),
        dma((2,)), dma((2,)),
        dma((Z,)), dma((Z,)),
        dma((CORES * G,)), dma((CORES * G,)),
        dma((Z,)), dma((Z,)),
        dma((CORES * G,)), dma((CORES * G,)),
        dma((Z,)), dma((Z,)),
        dma((CORES * G,)), dma((CORES * G,)),
    ]
    out = pl.pallas_call(
        functools.partial(kernel, G, C),
        out_shape=(
            pltpu.VMEM((2, R, W, K), f32),
            pltpu.VMEM((2, R, W, K), f32),
            pltpu.VMEM((2, own), f32),
            pltpu.VMEM((1, T), f32),
        ),
        in_specs=[pl.BlockSpec(memory_space=pltpu.HBM)] * 7,
        out_specs=(vmem,) * 4,
        scratch_shapes=scratch,
        compiler_params=pltpu.CompilerParams(
            collective_id=0, has_side_effects=True, vmem_limit_bytes=60 * 1024 * 1024
        ),
    )(density, susceptibility, station_cell, station_line, observed, data_weight, trial_steps)
    out = pl.pallas_call(
        deliver,
        out_shape=tuple(jax.ShapeDtypeStruct(x.shape, x.dtype) for x in out),
        in_specs=[vmem] * 4,
        out_specs=(pl.BlockSpec(memory_space=pltpu.HBM),) * 4,
        scratch_shapes=[dma((4,))],
        compiler_params=pltpu.CompilerParams(vmem_limit_bytes=1024 * 1024),
    )(*out)
    return out[0], out[1], out[2], out[3].reshape(-1)


def solution(mesh):
    placed = (
        P("gx", "gy", None),
        P("gx", "gy", None),
        P(None, "gx"),
        P(None, "gx"),
        P(None, "gx"),
        P(None, "gx"),
        P(),
    )
    return jax.shard_map(
        functools.partial(body, mesh.shape["gx"], mesh.shape["gy"]),
        mesh=mesh,
        in_specs=placed,
        out_specs=(P(None, "gx", "gy", None), P(None, "gx", "gy", None), P(None, "gx"), P()),
        check_vma=False,
    )
```
